32 devices in a mesh: node: 4 (over y, x), intra: 8 (over z, core).
Axes of the slice: x: 2, y: 2, z: 4, core: 2. Of those that a mesh axis runs over, the one named last changes fastest.
Arguments:
- gradients: bfloat16 [4, 8, 3072, 512], P('node', 'intra'), as said below
- sign_table: int32 [64, 512], replicated, may hold values from -1 to 1, as said below
- loss_scale: float32 [1], replicated, may hold values from 256 to 65536
- step_count: int32 [1], replicated, may hold values from 1 to 8
- weights: float32 [3072, 512], P('intra', 'node'), may hold values from -6 to 6
- first_moment: float32 [3072, 512], P('intra', 'node'), may hold values from -3 to 3
- second_moment: float32 [3072, 512], P('intra', 'node'), may hold values from 0.01 to 0.1
Outputs:
- new_weights: float32 [3072, 512], P('intra', 'node')
- new_first: float32 [3072, 512], P('intra', 'node')
- new_second: float32 [3072, 512], P('intra', 'node')
The draws below stay inside these ranges and needn't reach their ends.
Inputs may be any that keep to these rules, and one draw needn't show every extreme that they name: `gradients`: each replica's gradient is multiplied by loss_scale. `sign_table`: every entry is -1 or 1.
All inputs are finite; a program needn't handle non-finite values.
Results may differ from the reference program's by a relative error of at most 0.0003.
Values sent between devices are 32-bit elements; how exact they have to be, the bound alone decides.
A program may use at most 128 MiB of HBM per device.

```python
import math
import jax
import jax.numpy as jnp
from jax import lax

BLOCK = 128
SIGN_ROWS = 64
GRAD_ROWS = 3072
GRAD_COLS = 512
N_NODE = 4
N_INTRA = 8


def shared_scale(key):
    fraction = jax.random.uniform(jax.random.fold_in(key, 11), (), jnp.float32)
    return jnp.exp(jnp.log(256.0) + fraction * (jnp.log(65536.0) - jnp.log(256.0)))


def draw_loss_scale(key, part):
    return shared_scale(key).reshape(1).astype(jnp.float32)


def draw_gradients(key, part):
    replicas = N_NODE * N_INTRA
    ranking = jnp.arange(replicas, dtype=jnp.float32) / (replicas - 1)
    jitter = jax.random.uniform(jax.random.fold_in(key, 1), (replicas,), jnp.float32, 0.8, 1.25)
    device_scale = jnp.power(3.0, ranking) * jitter
    noise = jax.random.truncated_normal(jax.random.fold_in(key, 2), -6.0, 6.0, (replicas, GRAD_ROWS, GRAD_COLS), jnp.float32)
    values = noise * device_scale[:, None, None] * shared_scale(key)
    return values.reshape(N_NODE, N_INTRA, GRAD_ROWS, GRAD_COLS).astype(jnp.bfloat16)


def draw_sign_table(key, part):
    return 2 * jax.random.randint(jax.random.fold_in(key, 21), (SIGN_ROWS, GRAD_COLS), 0, 2, jnp.int32) - 1


def level_of(rng, dims, cuts, low, high):
    def one(position, blocks):
        steps = jax.random.uniform(jax.random.fold_in(jax.random.fold_in(rng, 6), position), (blocks,), jnp.float32, low / len(cuts), high / len(cuts))
        return jnp.repeat(jnp.exp(steps), dims[position] // blocks).reshape((-1,) + (1,) * (len(dims) - position - 1))

    loudness = one(*cuts[0])
    for cut in cuts[1:]:
        loudness = loudness * one(*cut)
    return loudness


def bell_draw(key, shape, scale, most, cuts=(), held_as=jnp.bfloat16):
    level = level_of(key, shape, cuts, -0.22, 0.18) if cuts else 1.0
    array = jax.random.normal(key, shape, jnp.float32) * scale * level
    return jnp.minimum(jnp.maximum(array, -most), most).astype(held_as)


def setup_inputs(seed: int = 0) -> dict:
    arg_keys = jax.random.split(jax.random.key(seed), 8)
    return {
        "gradients": draw_gradients(jax.random.fold_in(arg_keys[7], 71), 0),
        "sign_table": draw_sign_table(jax.random.fold_in(arg_keys[7], 71), 0),
        "loss_scale": draw_loss_scale(jax.random.fold_in(arg_keys[7], 71), 0),
        "step_count": jax.random.randint(arg_keys[3], (1,), 1, 9).astype(jnp.int32),
        "weights": bell_draw(arg_keys[4], (GRAD_ROWS, GRAD_COLS), 1.0, 6.0, ((0, 8), (1, 4)), jnp.float32),
        "first_moment": bell_draw(arg_keys[5], (GRAD_ROWS, GRAD_COLS), 0.2, 3.0, ((0, 8), (1, 4)), jnp.float32),
        "second_moment": jnp.clip(jnp.exp(math.log(0.1) - 2.3025851 * jax.random.uniform(arg_keys[6], (GRAD_ROWS, GRAD_COLS), jnp.float32) ** level_of(arg_keys[6], (GRAD_ROWS, GRAD_COLS), ((0, 8), (1, 4)), -0.2, 0.2)), 0.01, 0.1),
    }


def hadamard(order):
    index = jnp.arange(order, dtype=jnp.int32)
    common = index[:, None] & index[None, :]
    parity = jnp.zeros((order, order), jnp.int32)
    for bit_index in range(order.bit_length() - 1):
        parity = parity ^ common >> bit_index & 1
    return 1 - 2 * parity

def reference(gradients, sign_table, loss_scale, step_count, weights, first_moment, second_moment):
    table_int = hadamard(BLOCK)
    table_half = table_int.astype(jnp.bfloat16)
    table_full = table_int.astype(jnp.float32)
    inverse_root = 1.0 / math.sqrt(BLOCK)
    sign_tile = jnp.tile(sign_table, (GRAD_ROWS // SIGN_ROWS, 1))
    sign_half = sign_tile.astype(jnp.bfloat16)
    replicas = gradients.reshape(N_NODE * N_INTRA, GRAD_ROWS, GRAD_COLS)

    def rotate(replica):
        signed = (replica * sign_half).reshape(-1, BLOCK)
        spun = jnp.dot(signed, table_half, preferred_element_type=jnp.float32) * inverse_root
        return spun.reshape(GRAD_ROWS, GRAD_COLS)
    maxima = lax.map(lambda replica: jnp.max(jnp.abs(rotate(replica))), replicas)
    top_value = jnp.max(maxima)
    level_scale = 127.0 / top_value

    def accumulate(carry, replica):
        levels = jnp.floor(rotate(replica) * level_scale + 0.5)
        return (carry + levels, None)
    summed, _ = lax.scan(accumulate, jnp.zeros((GRAD_ROWS, GRAD_COLS), jnp.float32), replicas)
    factor = top_value / (127.0 * (N_NODE * N_INTRA) * loss_scale[0])
    scaled = (summed * factor).reshape(-1, BLOCK)
    back = jnp.dot(scaled, table_full, precision=lax.Precision.HIGHEST) * inverse_root
    grad = back.reshape(GRAD_ROWS, GRAD_COLS) * sign_tile.astype(jnp.float32)
    new_first = 0.9 * first_moment + 0.1 * grad
    new_second = 0.95 * second_moment + 0.05 * grad * grad
    steps_float = step_count[0].astype(jnp.float32)
    first_hat = new_first / (1.0 - jnp.power(jnp.float32(0.9), steps_float))
    second_hat = new_second / (1.0 - jnp.power(jnp.float32(0.95), steps_float))
    update = first_hat / (jnp.sqrt(second_hat) + 1e-08) + 0.1 * weights
    new_weights = weights - 0.2 * update
    return (new_weights, new_first, new_second)
```

```python
import contextlib
import functools
import math

import jax
import jax.numpy as jnp
from jax import lax
from jax.experimental import pallas as pl
from jax.experimental.pallas import tpu as pltpu
from jax.sharding import PartitionSpec as P

BLOCK = 128
WIDE = 2 * BLOCK
SIGN_ROWS = 64
CORES = 2
SLOTS = 8
SUBS = 2
CHUNKS = 3
ROOT = 1.0 / math.sqrt(BLOCK)
MESH = pl.DeviceIdType.MESH


def scope(name):
    return contextlib.nullcontext()


def parity_sign(rows, columns):
    common = lax.broadcasted_iota(jnp.int32, (rows, columns), 0) & lax.broadcasted_iota(
        jnp.int32, (rows, columns), 1
    ) & (BLOCK - 1)
    parity = common
    for bit_index in range(1, BLOCK.bit_length() - 1):
        parity = parity ^ (common >> bit_index)
    return (1 - 2 * (parity & 1)).astype(jnp.float32)


def paired_table():
    row = lax.broadcasted_iota(jnp.int32, (WIDE, WIDE), 0) // BLOCK
    column = lax.broadcasted_iota(jnp.int32, (WIDE, WIDE), 1) // BLOCK
    return jnp.where(row == column, parity_sign(WIDE, WIDE), 0.0).astype(jnp.bfloat16)


def plan_rows(owned):
    z_rows = owned * 5 // 24 // 16 * 16
    return z_rows, (owned - z_rows) // 2


def reduce_kernel(
    n_node, n_intra, grad_ref, sign_ref, scale_ref, step_ref, weight_ref, first_ref, second_ref,
    sum_ref, aux_ref, sign_out, weight_out, first_out, second_out,
    stage, sign_tab, sign_bf, table_bf, lev, levz, pair, pairz, raw, zraw, first, second, third, agg,
    zin, zfirst, zsecond, peaks,
    load_sem, side_sem, pair_send, pair_recv, pairz_send, pairz_recv, raw_send, raw_recv,
    zraw_send, zraw_recv, first_send, first_recv, second_send, second_recv, third_send, third_recv,
    agg_send, agg_recv, zin_send, zin_recv, zfirst_send, zfirst_recv, zsecond_send, zsecond_recv,
    peak_send, peak_recv,
):
    n_z = n_intra // CORES
    last = n_z - 1
    n_dev = n_node * n_intra
    owned = sum_ref.shape[0]
    z_rows, half = plan_rows(owned)
    zh = z_rows // 2
    cut = (half // SUBS + 7) // 8 * 8
    spans = ((0, cut), (cut, half - cut))
    raw_rows = half * 7 // 10 // 8 * 8
    raw_spans = ((0, raw_rows), (raw_rows, half - raw_rows))
    node, intra = lax.axis_index("node"), lax.axis_index("intra")
    z, core = intra // CORES, intra % CORES
    hi, lo = node // 2, node % 2
    me = node * n_intra + intra
    end = (z == 0) | (z == last)
    near = (z == 1) | (z == last - 1)
    inward = jnp.where(z == 0, 1, last - 1)

    def at(node_index, z_index, core_index):
        return (node_index, z_index * CORES + core_index)

    def flat(index):
        return (index // n_intra, index % n_intra)

    def send(src, dst, send_sem, recv_sem, device):
        return pltpu.make_async_remote_copy(
            src_ref=src, dst_ref=dst, send_sem=send_sem, recv_sem=recv_sem,
            device_id=device, device_id_type=MESH,
        )

    def piece(k):
        lower = jnp.where(k < last - z, last - k, k - (last - z))
        upper = jnp.where(k < z, k, last - (k - z))
        return jnp.where(z < n_z // 2, lower, upper)

    def block_at(q):
        return piece(q // CORES) * CORES + jnp.where(q % CORES == 0, core, 1 - core)

    def load(q):
        slot = lax.rem(q, SLOTS)
        return pltpu.make_async_copy(
            grad_ref.at[pl.ds(block_at(q) * owned, owned)], stage.at[slot], load_sem.at[slot]
        )

    sides = [
        pltpu.make_async_copy(src, dst, side_sem.at[n])
        for n, (src, dst) in enumerate((
            (sign_ref, sign_tab), (weight_ref, weight_out), (first_ref, first_out), (second_ref, second_out),
        ))
    ]
    sides[0].start()
    for q in range(min(SLOTS, n_intra)):
        load(q).start()
    for copy in sides[1:]:
        copy.start()

    barrier = pltpu.get_barrier_semaphore()

    def greet(step, carry):
        pl.semaphore_signal(
            barrier, inc=1, device_id=flat(lax.rem(me + step, n_dev)), device_id_type=MESH
        )
        return carry

    lax.fori_loop(1, n_dev, greet, 0)
    table_bf[...] = paired_table()
    with scope("Asign"):
        sides[0].wait()
        sign_bf[...] = sign_tab[...].astype(jnp.float32).astype(jnp.bfloat16)

    def rotate(q, most):
        load(q).wait()
        i = block_at(q)
        block = stage[lax.rem(q, SLOTS)]
        for w in range(n_node // 2):
            cols = slice(w * WIDE, (w + 1) * WIDE)
            part = block[:, cols].reshape(owned // SIGN_ROWS, SIGN_ROWS, WIDE)
            signed = (part * sign_bf[:, cols][None]).reshape(owned, WIDE)
            both = jnp.dot(signed, table_bf[...], preferred_element_type=jnp.float32)
            for v in range(2):
                spun = both[:, v * BLOCK : (v + 1) * BLOCK]
                for h in range(2):
                    lev[i, w, v, h] = spun[h * half : (h + 1) * half]
                levz[i, w, v] = spun[2 * half :]
                most = jnp.maximum(
                    most, jnp.max(jnp.abs(spun).reshape(owned // 8, 8, BLOCK), axis=0)
                )

        @pl.when(q + SLOTS < n_intra)
        def _():
            load(q + SLOTS).start()

        return most

    lo_peer = hi * 2 + 1 - lo
    hi_peer = (1 - hi) * 2 + lo

    def pair_copy(p):
        other = p * CORES + 1 - core
        return send(
            lev.at[other], pair.at[p], pair_send.at[p], pair_recv.at[p], at(node, z, 1 - core)
        )

    def pairz_copy(p):
        other = p * CORES + 1 - core
        return send(
            levz.at[other], pairz.at[p], pairz_send.at[p], pairz_recv.at[p], at(node, z, 1 - core)
        )

    def raw_copies(flip):
        target = core if flip == 0 else 1 - core
        i, r = piece(0) * CORES + target, pl.ds(0, raw_rows)
        return [
            send(
                src, raw.at[flip, h], raw_send.at[flip, h], raw_recv.at[flip, h],
                at(peer, z, target),
            )
            for h, src, peer in (
                (0, lev.at[i, :, 1 - lo, 0, r], lo_peer),
                (1, lev.at[i, 1 - hi, :, 1, r], hi_peer),
            )
        ]

    def zraw_copy(flip):
        target = core if flip == 0 else 1 - core
        return send(
            levz.at[piece(0) * CORES + target, :, :, z_part(0)], zraw.at[flip], zraw_send.at[flip], zraw_recv.at[flip],
            at(node, inward, target),
        )

    def rows_of(s, lead=False):
        return pl.ds(*(raw_spans if lead else spans)[s])

    def first_copies(p, s, lead=False):
        i, r = p * CORES + core, rows_of(s, lead)
        return [
            send(
                src, first.at[p, h, :, r], first_send.at[h, p * SUBS + s],
                first_recv.at[h, p * SUBS + s], at(peer, z, core),
            )
            for h, src, peer in (
                (0, lev.at[i, :, 1 - lo, 0, r], lo_peer),
                (1, lev.at[i, 1 - hi, :, 1, r], hi_peer),
            )
        ]

    def second_copies(p, s, lead=False):
        i, r = p * CORES + core, rows_of(s, lead)
        return [
            send(
                src, second.at[p, h, r], second_send.at[h, p * SUBS + s],
                second_recv.at[h, p * SUBS + s], at(peer, z, core),
            )
            for h, src, peer in (
                (0, lev.at[i, 1 - hi, lo, 0, r], hi_peer),
                (1, lev.at[i, hi, 1 - lo, 1, r], lo_peer),
            )
        ]

    def third_copy(p, slot, s):
        r = rows_of(s)
        return send(
            lev.at[p * CORES + core, hi, lo, :, r], third.at[slot, :, r],
            third_send.at[p * SUBS + s], third_recv.at[slot * SUBS + s], at(node, p, core),
        )

    def agg_copy(s):
        r = rows_of(s)
        return send(
            lev.at[piece(0) * CORES + core, hi, lo, :, r], agg.at[:, r], agg_send.at[s], agg_recv.at[s],
            at(node, inward, core),
        )

    def z_part(h):
        return pl.ds(h * zh, zh)

    def z_copy(p, h):
        onward = jnp.where(p > z, z + 1, z - 1)
        slot = jnp.where((p < z) & (p == onward), n_z, p)
        return send(
            levz.at[p * CORES + core, :, :, z_part(h)], zin.at[slot, :, :, z_part(h)],
            zin_send.at[p * 2 + h], zin_recv.at[slot * 2 + h], at(node, onward, core),
        )

    def z_arrived(slot, h):
        send(
            levz.at[core, :, :, z_part(h)], zin.at[slot, :, :, z_part(h)],
            zin_send.at[0], zin_recv.at[slot * 2 + h], at(node, inward, core),
        ).wait_recv()

    def z_first_copies():
        return [
            send(src, zfirst.at[h], zfirst_send.at[h], zfirst_recv.at[h], at(peer, z, core))
            for h, src, peer in (
                (0, levz.at[intra, :, 1 - lo, z_part(0)], lo_peer),
                (1, levz.at[intra, 1 - hi, :, z_part(1)], hi_peer),
            )
        ]

    def z_second_copies():
        return [
            send(src, zsecond.at[h], zsecond_send.at[h], zsecond_recv.at[h], at(peer, z, core))
            for h, src, peer in (
                (0, levz.at[intra, 1 - hi, lo, z_part(0)], hi_peer),
                (1, levz.at[intra, hi, 1 - lo, z_part(1)], lo_peer),
            )
        ]

    def peak_copy(target, slot):
        return send(
            peaks.at[slot], peaks.at[slot], peak_send.at[target], peak_recv.at[slot], flat(target)
        )

    with scope("A_rotate"):
        most = lax.fori_loop(0, n_intra, rotate, jnp.zeros((8, BLOCK), jnp.float32))
        peaks[me] = jnp.max(most, axis=0, keepdims=True)
    with scope("B_barrier"):
        pl.semaphore_wait(barrier, n_dev - 1)

    def tell(step, carry):
        peak_copy(lax.rem(me + step, n_dev), me).start()
        return carry

    with scope("C_issue"):
        lax.fori_loop(1, n_dev, tell, 0)
        for flip in range(2):
            for copy in raw_copies(flip):
                copy.start()

        @pl.when(end)
        def _():
            for flip in range(2):
                zraw_copy(flip).start()

        def share(k, carry):
            pair_copy(piece(k)).start()
            pairz_copy(piece(k)).start()
            return carry

        lax.fori_loop(0, n_z, share, 0)

    with scope("D_sides"):
        for copy in sides[1:]:
            copy.wait()
        ones = jnp.ones((1, BLOCK), jnp.float32)
        steps = ones * step_ref[0].astype(jnp.float32)
        aux_ref[0:1] = 1.0 / (1.0 - jnp.exp(steps * math.log(0.9)))
        aux_ref[1:2] = 1.0 / (1.0 - jnp.exp(steps * math.log(0.95)))

    def hear(step, carry):
        other = lax.rem(me + step, n_dev)
        peak_copy(other, other).wait_recv()
        return carry

    with scope("E_peaks"):
        lax.fori_loop(1, n_dev, hear, 0)
        tops = jnp.max(peaks[...], axis=0)
        top_value = jnp.max(tops, axis=1, keepdims=True) * ROOT
        level_scale = 127.0 / top_value
        factor = (ones * top_value) / (ones * (127.0 * float(n_dev) * scale_ref[0]))
        column = pl.multiple_of(node * BLOCK, BLOCK)
        sign_out[...] = sign_tab[:, pl.ds(column, BLOCK)].astype(jnp.float32) * (factor * ROOT)

    def level(value):
        return jnp.floor((value * ROOT) * level_scale + 0.5)

    def level_piece(k, s, lead=False):
        p = piece(k)
        i, r = p * CORES + core, rows_of(s, lead)
        if lead or (s == 0):
            pair_copy(p).wait_recv()
        for j in range(n_node):
            for h in range(2):
                spot = (j // 2, j % 2, h, r)
                lev[(i,) + spot] = level(lev[(i,) + spot]) + level(pair[(p,) + spot])
        for copy in first_copies(p, s, lead):
            copy.start()

    def first_sum(k, s, lead=False):
        p = piece(k)
        i, r = p * CORES + core, rows_of(s, lead)
        for copy in first_copies(p, s, lead):
            copy.wait_recv()
        for j in range(2):
            lev[i, j, lo, 0, r] = lev[i, j, lo, 0, r] + first[p, 0, j, r]
            lev[i, hi, j, 1, r] = lev[i, hi, j, 1, r] + first[p, 1, j, r]
        for copy in second_copies(p, s, lead):
            copy.start()

    def second_sum(k, s, lead=False):
        p = piece(k)
        i, r = p * CORES + core, rows_of(s, lead)
        for copy in second_copies(p, s, lead):
            copy.wait_recv()
        for h in range(2):
            lev[i, hi, lo, h, r] = lev[i, hi, lo, h, r] + second[p, h, r]

    def raw_piece():
        p = piece(0)
        i, r = p * CORES + core, rows_of(0, True)
        for flip in range(2):
            for copy in raw_copies(flip):
                copy.wait_recv()

        def kept(h, j, spot):
            lev[(i,) + spot] = (
                level(lev[(i,) + spot]) + level(pair[(p,) + spot])
                + level(raw[0, h, j]) + level(raw[1, h, j])
            )

        for j in range(2):
            kept(0, j, (j, lo, 0, r))
            kept(1, j, (hi, j, 1, r))
        for copy in second_copies(p, 0, True):
            copy.start()

    def z_level(p, h, wait):
        i, r = p * CORES + core, z_part(h)
        if wait:
            pairz_copy(p).wait_recv()
        for j in range(n_node):
            spot = (j // 2, j % 2, r)
            levz[(i,) + spot] = level(levz[(i,) + spot]) + level(pairz[(p,) + spot])

    def z_add(p, slot, h):
        i, r = p * CORES + core, z_part(h)
        z_arrived(slot, h)
        for j in range(n_node):
            spot = (j // 2, j % 2, r)
            levz[(i,) + spot] = levz[(i,) + spot] + zin[(slot,) + spot]

    def z_pass(k, h):
        p = piece(k)
        z_level(p, h, h == 0)
        z_add(p, p, h)
        z_copy(p, h).start()

    def z_inner(k, h):
        @pl.when(jnp.logical_not(end))
        def _():
            z_pass(k, h)

    def z_lead():
        @pl.when(end)
        def _():
            z_level(piece(0), 1, True)
            z_copy(piece(0), 1).start()

        @pl.when(near)
        def _():
            p = piece(0)
            i, r = p * CORES + core, z_part(0)
            z_level(p, 0, True)
            for flip in range(2):
                zraw_copy(flip).wait_recv()
            for j in range(n_node):
                spot = (j // 2, j % 2)
                levz[(i,) + spot + (r,)] = (
                    levz[(i,) + spot + (r,)]
                    + level(zraw[(0,) + spot]) + level(zraw[(1,) + spot])
                )
            z_copy(p, 0).start()

        @pl.when(jnp.logical_not(end | near))
        def _():
            z_pass(0, 0)

    def z_ahead(k):
        @pl.when(end & (k < last))
        def _():
            p = piece(k)
            for h in range(2):
                z_level(p, h, h == 0)
                z_copy(p, h).start()

    with scope("F0"):
        level_piece(0, 1, True)
        z_lead()
        level_piece(1, 0)
        z_ahead(1)
        raw_piece()
    with scope("F1"):
        z_inner(0, 1)
        level_piece(1, 1)
        z_ahead(2)
        first_sum(0, 1, True)
        second_sum(0, 0, True)
        z_inner(1, 0)
        first_sum(1, 0)
        second_sum(0, 1, True)

        @pl.when(end)
        def _():
            for s in range(SUBS):
                agg_copy(s).start()

        @pl.when(jnp.logical_not(end | near))
        def _():
            for s in range(SUBS):
                third_copy(piece(0), z, s).start()

    def z_finish():
        for h in range(2):
            z_level(z, h, h == 0)

            @pl.when(z > 0)
            def _():
                z_add(z, z, h)

            @pl.when(z < last)
            def _():
                z_add(z, n_z, h)

        for copy in z_first_copies():
            copy.start()

    def pipeline(k, carry):
        for s in range(SUBS):
            with scope("G%d" % s):
                level_piece(k, s)
                z_ahead(1 + (k - 1) * SUBS + s)
                if s == 0:
                    first_sum(k - 1, 1)

                    @pl.when(k < last)
                    def _():
                        z_inner(k - 1, 1)

                    @pl.when((k == last) & near)
                    def _():
                        p = piece(0)
                        i = p * CORES + core
                        for part in range(SUBS):
                            r = rows_of(part)
                            agg_copy(part).wait_recv()
                            for h in range(2):
                                lev[i, hi, lo, h, r] = lev[i, hi, lo, h, r] + agg[h, r]
                            third_copy(p, z, part).start()
                else:
                    first_sum(k, 0)

                    @pl.when(k < last)
                    def _():
                        z_inner(k, 0)

                    @pl.when(k == last - 1)
                    def _():
                        z_inner(k, 1)

                with scope("Gs"):
                    second_sum(k - 1, s)
                third_copy(piece(k - 1), z, s).start()
        return carry

    lax.fori_loop(2, n_z, pipeline, 0)
    with scope("H_zfinal"):
        z_finish()
    with scope("I_tail"):
        first_sum(last, 1)
        second_sum(last, 0)
    with scope("J_ztail"):
        for copy in z_first_copies():
            copy.wait_recv()
        for j in range(2):
            levz[intra, j, lo, z_part(0)] = levz[intra, j, lo, z_part(0)] + zfirst[0, j]
            levz[intra, hi, j, z_part(1)] = levz[intra, hi, j, z_part(1)] + zfirst[1, j]
        for copy in z_second_copies():
            copy.start()
    with scope("K_last"):
        second_sum(last, 1)

    def from_plane(step, carry):
        other = lax.rem(z + step, n_z)

        @pl.when(jnp.abs(other - z) != last)
        def _():
            for s in range(SUBS):
                r = rows_of(s)
                third_copy(other, other, s).wait_recv()
                for h in range(2):
                    lev[intra, hi, lo, h, r] = lev[intra, hi, lo, h, r] + third[other, h, r]

        return carry

    with scope("L_third"):
        lax.fori_loop(1, n_z, from_plane, 0)
        for h in range(2):
            sum_ref[h * half : (h + 1) * half] = lev[intra, hi, lo, h]
    with scope("M_zlast"):
        for copy in z_second_copies():
            copy.wait_recv()
        for h in range(2):
            sum_ref[2 * half + h * zh : 2 * half + (h + 1) * zh] = (
                levz[intra, hi, lo, z_part(h)] + zsecond[h]
            )

    def told(step, carry):
        peak_copy(lax.rem(me + step, n_dev), me).wait_send()
        return carry

    def finish(k, carry):
        p = piece(k)
        pair_copy(p).wait_send()
        pairz_copy(p).wait_send()

        @pl.when(k > 0)
        def _():
            for s in range(SUBS):
                for copy in first_copies(p, s) + second_copies(p, s):
                    copy.wait_send()

        @pl.when(k < last)
        def _():
            z_copy(p, 1).wait_send()

        @pl.when((k < last) & jnp.logical_not(end & (k == 0)))
        def _():
            z_copy(p, 0).wait_send()
            for s in range(SUBS):
                third_copy(p, z, s).wait_send()

        return carry

    with scope("N_finish"):
        lax.fori_loop(1, n_dev, told, 0)
        for flip in range(2):
            for copy in raw_copies(flip):
                copy.wait_send()
        p = piece(0)
        for copy in first_copies(p, 1, True) + second_copies(p, 0, True) + second_copies(p, 1, True):
            copy.wait_send()

        @pl.when(end)
        def _():
            for flip in range(2):
                zraw_copy(flip).wait_send()
            for s in range(SUBS):
                agg_copy(s).wait_send()

        lax.fori_loop(0, n_z, finish, 0)
        for copy in z_first_copies() + z_second_copies():
            copy.wait_send()


def adam_kernel(
    sum_ref, aux_ref, sign_ref, weight_ref, first_ref, second_ref,
    new_weight_ref, new_first_ref, new_second_ref, weight_buf, first_buf, second_buf, sems,
):
    owned = sum_ref.shape[0]
    table = parity_sign(WIDE, BLOCK)
    upper = lax.broadcasted_iota(jnp.int32, (WIDE, BLOCK), 0) < BLOCK
    table = jnp.where(upper, table * 64.0, table).astype(jnp.bfloat16)
    signs = sign_ref[...]
    first_unbias, second_unbias = aux_ref[0:1], aux_ref[1:2]
    rows = owned // CHUNKS
    copies = []
    for c in range(CHUNKS):
        r = slice(c * rows, (c + 1) * rows)
        summed = sum_ref[r]
        high = jnp.floor(summed * (1.0 / 64.0))
        low = summed - high * 64.0
        both = jnp.concatenate([high, low], axis=1).astype(jnp.bfloat16)
        back = jnp.dot(both, table, preferred_element_type=jnp.float32)
        grad = (back.reshape(rows // SIGN_ROWS, SIGN_ROWS, BLOCK) * signs[None]).reshape(rows, BLOCK)
        new_first = 0.9 * first_ref[r] + 0.1 * grad
        new_second = 0.95 * second_ref[r] + 0.05 * grad * grad
        first_buf[r] = new_first
        second_buf[r] = new_second
        weights = weight_ref[r]
        update = (new_first * first_unbias) / (jnp.sqrt(new_second * second_unbias) + 1e-08)
        weight_buf[r] = weights - 0.2 * (update + 0.1 * weights)
        for n, (src, dst) in enumerate((
            (first_buf, new_first_ref), (second_buf, new_second_ref), (weight_buf, new_weight_ref),
        )):
            copy = pltpu.make_async_copy(src.at[r], dst.at[r], sems.at[n, c])
            copy.start()
            copies.append(copy)
    for copy in copies:
        copy.wait()


def shards(gradients, sign_table, loss_scale, step_count, weights, first_moment, second_moment):
    n_node, n_intra = lax.axis_size("node"), lax.axis_size("intra")
    n_z = n_intra // CORES
    n_dev = n_node * n_intra
    local = gradients.reshape(gradients.shape[2:])
    rows, columns = local.shape
    owned = weights.shape[0]
    z_rows, half = plan_rows(owned)
    zh = z_rows // 2
    n_hi = n_node // 2
    anywhere = pl.BlockSpec(memory_space=pl.ANY)
    smem = pl.BlockSpec(memory_space=pltpu.SMEM)
    hbm = functools.partial(pltpu.with_memory_space_constraint, memory_space=pltpu.HBM)
    vmem = pl.BlockSpec(memory_space=pltpu.VMEM)
    dma = pltpu.SemaphoreType.DMA
    f32 = jnp.float32
    slots = min(SLOTS, n_intra)
    buffers = [
        ((slots, owned, columns), jnp.bfloat16),
        ((SIGN_ROWS, columns), jnp.int32),
        ((SIGN_ROWS, columns), jnp.bfloat16),
        ((WIDE, WIDE), jnp.bfloat16),
    ]
    large = [
        ((n_intra, n_hi, 2, 2, half, BLOCK), f32),
        ((n_intra, n_hi, 2, z_rows, BLOCK), f32),
        ((n_z, n_hi, 2, 2, half, BLOCK), f32),
        ((n_z, n_hi, 2, z_rows, BLOCK), f32),
        ((2, 2, 2, half * 7 // 10 // 8 * 8, BLOCK), f32),
        ((2, n_hi, 2, zh, BLOCK), f32),
        ((n_z, 2, 2, half, BLOCK), f32),
        ((n_z, 2, half, BLOCK), f32),
        ((n_z, 2, half, BLOCK), f32),
        ((2, half, BLOCK), f32),
        ((n_z + 1, n_hi, 2, z_rows, BLOCK), f32),
        ((2, 2, zh, BLOCK), f32),
        ((2, zh, BLOCK), f32),
        ((n_dev, 1, BLOCK), f32),
    ]
    held = sum(math.prod(shape) * jnp.dtype(kind).itemsize for shape, kind in buffers + large)
    shape = (owned, BLOCK)
    outs = pl.pallas_call(
        functools.partial(reduce_kernel, n_node, n_intra),
        out_shape=(
            pltpu.VMEM(shape, f32), pltpu.VMEM((8, BLOCK), f32), pltpu.VMEM((SIGN_ROWS, BLOCK), f32),
            pltpu.VMEM(shape, f32), pltpu.VMEM(shape, f32), pltpu.VMEM(shape, f32),
        ),
        in_specs=[anywhere] * 2 + [smem] * 2 + [anywhere] * 3,
        out_specs=(vmem,) * 6,
        scratch_shapes=[pltpu.VMEM(*b) for b in buffers]
        + [pltpu.VMEM(*b) for b in large]
        + [
            dma((slots,)), dma((4,)),
            dma((n_z,)), dma((n_z,)), dma((n_z,)), dma((n_z,)),
            dma((2, 2)), dma((2, 2)), dma((2,)), dma((2,)),
            dma((2, n_z * SUBS)), dma((2, n_z * SUBS)),
            dma((2, n_z * SUBS)), dma((2, n_z * SUBS)),
            dma((n_z * SUBS,)), dma((n_z * SUBS,)),
            dma((SUBS,)), dma((SUBS,)),
            dma((n_z * 2,)), dma((n_z * 2 + 2,)),
            dma((2,)), dma((2,)), dma((2,)), dma((2,)),
            dma((n_dev,)), dma((n_dev,)),
        ],
        compiler_params=pltpu.CompilerParams(
            collective_id=0, has_side_effects=True, vmem_limit_bytes=held + (6 << 20)
        ),
    )(*(hbm(x) for x in (local, sign_table)), loss_scale, step_count,
      *(hbm(x) for x in (weights, first_moment, second_moment)))
    out = jax.ShapeDtypeStruct(shape, f32)
    return pl.pallas_call(
        adam_kernel,
        out_shape=(out, out, out),
        in_specs=[vmem] * 6,
        out_specs=(anywhere,) * 3,
        scratch_shapes=[pltpu.VMEM(shape, f32)] * 3 + [dma((3, CHUNKS))],
        compiler_params=pltpu.CompilerParams(vmem_limit_bytes=4 << 20),
    )(*outs)


def solution(mesh):
    own = P("intra", "node")
    return jax.shard_map(
        shards,
        mesh=mesh,
        in_specs=(P("node", "intra", None, None), P(), P(), P(), own, own, own),
        out_specs=(own, own, own),
        check_vma=False,
    )
```

```python
import contextlib
import functools
import math

import jax
import jax.numpy as jnp
from jax import lax
from jax.experimental import pallas as pl
from jax.experimental.pallas import tpu as pltpu
from jax.sharding import PartitionSpec as P

BLOCK = 128
WIDE = 2 * BLOCK
SIGN_ROWS = 64
CORES = 2
SLOTS = 8
SUBS = 2
CHUNKS = 3
ROOT = 1.0 / math.sqrt(BLOCK)
MESH = pl.DeviceIdType.MESH


def scope(name):
    return contextlib.nullcontext()


def parity_sign():
    shape = (BLOCK, BLOCK)
    parity = common = lax.broadcasted_iota(jnp.int32, shape, 0) & lax.broadcasted_iota(
        jnp.int32, shape, 1
    )
    for bit_index in range(1, BLOCK.bit_length() - 1):
        parity = parity ^ (common >> bit_index)
    return (1 - 2 * (parity & 1)).astype(jnp.float32)


def plan_rows(owned):
    z_rows = owned * 5 // 24 // 16 * 16
    return z_rows, (owned - z_rows) // 2


def reduce_kernel(
    n_node, n_intra, grad_ref, sign_ref, scale_ref, step_ref, weight_ref, first_ref, second_ref,
    sum_ref, aux_ref, sign_out, weight_out, first_out, second_out,
    stage, sign_tab, sign_bf, table_bf, lev, levz, pair, pairz, raw, zraw, first, second, third, agg,
    zin, zfirst, zsecond, peaks,
    load_sem, side_sem, pair_send, pair_recv, pairz_send, pairz_recv, raw_send, raw_recv,
    zraw_send, zraw_recv, first_send, first_recv, second_send, second_recv, third_send, third_recv,
    agg_send, agg_recv, zin_send, zin_recv, zfirst_send, zfirst_recv, zsecond_send, zsecond_recv,
    peak_send, peak_recv,
):
    n_z = n_intra // CORES
    last = n_z - 1
    n_dev = n_node * n_intra
    owned = sum_ref.shape[0]
    z_rows, half = plan_rows(owned)
    zh = z_rows // 2
    cut = (half // SUBS + 7) // 8 * 8
    spans = ((0, cut), (cut, half - cut))
    raw_rows = half * 7 // 10 // 8 * 8
    raw_spans = ((0, raw_rows), (raw_rows, half - raw_rows))
    node, intra = lax.axis_index("node"), lax.axis_index("intra")
    z, core = intra // CORES, intra % CORES
    hi, lo = node // 2, node % 2
    me = node * n_intra + intra
    end = (z == 0) | (z == last)
    near = (z == 1) | (z == last - 1)
    inward = jnp.where(z == 0, 1, last - 1)

    def at(node_index, z_index, core_index):
        return (node_index, z_index * CORES + core_index)

    def send(src, dst, send_sem, recv_sem, device):
        return pltpu.make_async_remote_copy(
            src_ref=src, dst_ref=dst, send_sem=send_sem, recv_sem=recv_sem,
            device_id=device, device_id_type=MESH,
        )

    def piece(k):
        lower = jnp.where(k < last - z, last - k, k - (last - z))
        upper = jnp.where(k < z, k, last - (k - z))
        return jnp.where(z < n_z // 2, lower, upper)

    def block_at(q):
        return piece(q // CORES) * CORES + jnp.where(q % CORES == 0, core, 1 - core)

    def load(q):
        slot = lax.rem(q, SLOTS)
        return pltpu.make_async_copy(
            grad_ref.at[pl.ds(block_at(q) * owned, owned)], stage.at[slot], load_sem.at[slot]
        )

    sides = [
        pltpu.make_async_copy(src, dst, side_sem.at[n])
        for n, (src, dst) in enumerate((
            (sign_ref, sign_tab), (weight_ref, weight_out), (first_ref, first_out), (second_ref, second_out),
        ))
    ]
    sides[0].start()
    for q in range(CORES):
        load(q).start()

    barrier = pltpu.get_barrier_semaphore()

    def everyone():
        for k in range(n_z):
            p = piece(k)
            for turn in range(n_node):
                other = lax.rem(node + turn, n_node)
                for flip in range(CORES):
                    if (k, turn, flip) != (last, 0, 0):
                        yield at(other, p, core if flip == 0 else 1 - core)

    for device in everyone():
        pl.semaphore_signal(barrier, inc=1, device_id=device, device_id_type=MESH)
    for q in range(CORES, min(SLOTS, n_intra)):
        load(q).start()
    for copy in sides[1:]:
        copy.start()
    table = parity_sign().astype(jnp.bfloat16)
    for a in range(2):
        for b in range(2):
            table_bf[a * BLOCK : (a + 1) * BLOCK, b * BLOCK : (b + 1) * BLOCK] = (
                table if a == b else jnp.zeros_like(table)
            )
    with scope("Asign"):
        sides[0].wait()
        sign_bf[...] = sign_tab[...].astype(jnp.float32).astype(jnp.bfloat16)

    def rotate(m, most):
        with scope("Aw"):
            for q in range(CORES):
                load(m * CORES + q).wait()
        p = piece(m)
        blocks = [p * CORES + core, p * CORES + 1 - core]
        both_blocks = stage[pl.ds(lax.rem(m * CORES, SLOTS), CORES)].reshape(CORES * owned, -1)
        for w in range(n_node // 2):
            cols = slice(w * WIDE, (w + 1) * WIDE)
            part = both_blocks[:, cols].reshape(CORES * owned // SIGN_ROWS, SIGN_ROWS, WIDE)
            signed = (part * sign_bf[:, cols][None]).reshape(CORES * owned, WIDE)
            both = jnp.dot(signed, table_bf[...], preferred_element_type=jnp.float32)
            for c in range(CORES):
                for v in range(2):
                    spun = both[c * owned : (c + 1) * owned, v * BLOCK : (v + 1) * BLOCK]
                    for h in range(2):
                        lev[blocks[c], w, v, h] = spun[h * half : (h + 1) * half]
                    levz[blocks[c], w, v] = spun[2 * half :]
                    most = jnp.maximum(
                        most, jnp.max(jnp.abs(spun).reshape(owned // 8, 8, BLOCK), axis=0)
                    )
        for q in range(CORES):

            @pl.when(m * CORES + q + SLOTS < n_intra)
            def _():
                load(m * CORES + q + SLOTS).start()

        return most

    lo_peer = hi * 2 + 1 - lo
    hi_peer = (1 - hi) * 2 + lo

    def pair_copy(p):
        other = p * CORES + 1 - core
        return send(
            lev.at[other], pair.at[p], pair_send.at[p], pair_recv.at[p], at(node, z, 1 - core)
        )

    def pairz_copy(p):
        other = p * CORES + 1 - core
        return send(
            levz.at[other], pairz.at[p], pairz_send.at[p], pairz_recv.at[p], at(node, z, 1 - core)
        )

    def raw_copies(flip):
        target = core if flip == 0 else 1 - core
        i, r = piece(0) * CORES + target, pl.ds(0, raw_rows)
        return [
            send(
                src, raw.at[flip, h], raw_send.at[flip, h], raw_recv.at[flip, h],
                at(peer, z, target),
            )
            for h, src, peer in (
                (0, lev.at[i, :, 1 - lo, 0, r], lo_peer),
                (1, lev.at[i, 1 - hi, :, 1, r], hi_peer),
            )
        ]

    def zraw_copy(flip):
        target = core if flip == 0 else 1 - core
        return send(
            levz.at[piece(0) * CORES + target, :, :, z_part(0)], zraw.at[flip], zraw_send.at[flip], zraw_recv.at[flip],
            at(node, inward, target),
        )

    def rows_of(s, lead=False):
        return pl.ds(*(raw_spans if lead else spans)[s])

    def first_copies(p, s, lead=False):
        i, r = p * CORES + core, rows_of(s, lead)
        return [
            send(
                src, first.at[p, h, :, r], first_send.at[h, p * SUBS + s],
                first_recv.at[h, p * SUBS + s], at(peer, z, core),
            )
            for h, src, peer in (
                (0, lev.at[i, :, 1 - lo, 0, r], lo_peer),
                (1, lev.at[i, 1 - hi, :, 1, r], hi_peer),
            )
        ]

    def second_copies(p, s, lead=False):
        i, r = p * CORES + core, rows_of(s, lead)
        return [
            send(
                src, second.at[p, h, r], second_send.at[h, p * SUBS + s],
                second_recv.at[h, p * SUBS + s], at(peer, z, core),
            )
            for h, src, peer in (
                (0, lev.at[i, 1 - hi, lo, 0, r], hi_peer),
                (1, lev.at[i, hi, 1 - lo, 1, r], lo_peer),
            )
        ]

    def third_copy(p, slot, s, lead=False):
        r = rows_of(s, lead)
        return send(
            lev.at[p * CORES + core, hi, lo, :, r], third.at[slot, :, r],
            third_send.at[p * SUBS + s], third_recv.at[slot * SUBS + s], at(node, p, core),
        )

    def agg_copy(s):
        r = rows_of(s, True)
        return send(
            lev.at[piece(0) * CORES + core, hi, lo, :, r], agg.at[:, r], agg_send.at[s], agg_recv.at[s],
            at(node, inward, core),
        )

    def z_part(h):
        return pl.ds(h * zh, zh)

    def z_copy(p, h):
        onward = jnp.where(p > z, z + 1, z - 1)
        slot = jnp.where((p < z) & (p == onward), n_z, p)
        return send(
            levz.at[p * CORES + core, :, :, z_part(h)], zin.at[slot, :, :, z_part(h)],
            zin_send.at[p * 2 + h], zin_recv.at[slot * 2 + h], at(node, onward, core),
        )

    def z_arrived(slot, h):
        send(
            levz.at[core, :, :, z_part(h)], zin.at[slot, :, :, z_part(h)],
            zin_send.at[0], zin_recv.at[slot * 2 + h], at(node, inward, core),
        ).wait_recv()

    def z_first_copies():
        return [
            send(src, zfirst.at[h], zfirst_send.at[h], zfirst_recv.at[h], at(peer, z, core))
            for h, src, peer in (
                (0, levz.at[intra, :, 1 - lo, z_part(0)], lo_peer),
                (1, levz.at[intra, 1 - hi, :, z_part(1)], hi_peer),
            )
        ]

    def z_second_copies():
        return [
            send(src, zsecond.at[h], zsecond_send.at[h], zsecond_recv.at[h], at(peer, z, core))
            for h, src, peer in (
                (0, levz.at[intra, 1 - hi, lo, z_part(0)], hi_peer),
                (1, levz.at[intra, hi, 1 - lo, z_part(1)], lo_peer),
            )
        ]

    def peak_copy(device):
        return send(peaks.at[me], peaks.at[me], peak_send, peak_recv, device)

    def all_peaks():
        every = peaks.at[pl.ds(0, n_dev - 1)]
        return send(every, every, peak_send, peak_recv, at(node, z, 1 - core))

    with scope("A_rotate"):
        most = lax.fori_loop(0, n_z, rotate, jnp.zeros((8, BLOCK), jnp.float32))
        peaks[me] = jnp.max(most, axis=0, keepdims=True)
    with scope("B_barrier"):
        pl.semaphore_wait(barrier, n_dev - 1)

    with scope("C_issue"):
        for device in everyone():
            peak_copy(device).start()
        for flip in range(2):
            for copy in raw_copies(flip):
                copy.start()

        @pl.when(end)
        def _():
            for flip in range(2):
                zraw_copy(flip).start()

        def share(k, carry):
            pair_copy(piece(k)).start()
            pairz_copy(piece(k)).start()
            return carry

        lax.fori_loop(0, n_z, share, 0)

    with scope("D_sides"):
        for copy in sides[1:]:
            copy.wait()
        ones = jnp.ones((1, BLOCK), jnp.float32)
        steps = ones * step_ref[0].astype(jnp.float32)
        aux_ref[0:1] = 1.0 / (1.0 - jnp.exp(steps * math.log(0.9)))
        aux_ref[1:2] = 1.0 / (1.0 - jnp.exp(steps * math.log(0.95)))

    with scope("E_peaks"):
        all_peaks().wait_recv()
        tops = jnp.max(peaks[...], axis=0)
        top_value = jnp.max(tops, axis=1, keepdims=True) * ROOT
        level_scale = 127.0 / top_value
        factor = (ones * top_value) / (ones * (127.0 * float(n_dev) * scale_ref[0]))
        column = pl.multiple_of(node * BLOCK, BLOCK)
        sign_out[...] = sign_tab[:, pl.ds(column, BLOCK)].astype(jnp.float32) * (factor * ROOT)

    def level(value):
        return jnp.floor((value * ROOT) * level_scale + 0.5)

    def level_piece(k, s, lead=False):
        p = piece(k)
        i, r = p * CORES + core, rows_of(s, lead)
        if lead or (s == 0):
            pair_copy(p).wait_recv()
        for j in range(n_node):
            for h in range(2):
                spot = (j // 2, j % 2, h, r)
                lev[(i,) + spot] = level(lev[(i,) + spot]) + level(pair[(p,) + spot])
        for copy in first_copies(p, s, lead):
            copy.start()

    def first_sum(k, s, lead=False):
        p = piece(k)
        i, r = p * CORES + core, rows_of(s, lead)
        for copy in first_copies(p, s, lead):
            copy.wait_recv()
        for j in range(2):
            lev[i, j, lo, 0, r] = lev[i, j, lo, 0, r] + first[p, 0, j, r]
            lev[i, hi, j, 1, r] = lev[i, hi, j, 1, r] + first[p, 1, j, r]
        for copy in second_copies(p, s, lead):
            copy.start()

    def second_sum(k, s, lead=False):
        p = piece(k)
        i, r = p * CORES + core, rows_of(s, lead)
        for copy in second_copies(p, s, lead):
            copy.wait_recv()
        for h in range(2):
            lev[i, hi, lo, h, r] = lev[i, hi, lo, h, r] + second[p, h, r]

    def raw_piece():
        p = piece(0)
        i, r = p * CORES + core, rows_of(0, True)
        for flip in range(2):
            for copy in raw_copies(flip):
                copy.wait_recv()

        def kept(h, j, spot):
            lev[(i,) + spot] = (
                level(lev[(i,) + spot]) + level(pair[(p,) + spot])
                + level(raw[0, h, j]) + level(raw[1, h, j])
            )

        for j in range(2):
            kept(0, j, (j, lo, 0, r))
            kept(1, j, (hi, j, 1, r))
        for copy in second_copies(p, 0, True):
            copy.start()

    def z_level(p, h, wait):
        i, r = p * CORES + core, z_part(h)
        if wait:
            pairz_copy(p).wait_recv()
        for j in range(n_node):
            spot = (j // 2, j % 2, r)
            levz[(i,) + spot] = level(levz[(i,) + spot]) + level(pairz[(p,) + spot])

    def z_add(p, slot, h):
        i, r = p * CORES + core, z_part(h)
        z_arrived(slot, h)
        for j in range(n_node):
            spot = (j // 2, j % 2, r)
            levz[(i,) + spot] = levz[(i,) + spot] + zin[(slot,) + spot]

    def z_pass(k, h):
        p = piece(k)
        z_level(p, h, h == 0)
        z_add(p, p, h)
        z_copy(p, h).start()

    def z_inner(k, h):
        @pl.when(jnp.logical_not(end))
        def _():
            z_pass(k, h)

    def z_lead():
        @pl.when(end)
        def _():
            z_level(piece(0), 1, True)
            z_copy(piece(0), 1).start()

        @pl.when(near)
        def _():
            p = piece(0)
            i, r = p * CORES + core, z_part(0)
            z_level(p, 0, True)
            for flip in range(2):
                zraw_copy(flip).wait_recv()
            for j in range(n_node):
                spot = (j // 2, j % 2)
                levz[(i,) + spot + (r,)] = (
                    levz[(i,) + spot + (r,)]
                    + level(zraw[(0,) + spot]) + level(zraw[(1,) + spot])
                )
            z_copy(p, 0).start()

        @pl.when(jnp.logical_not(end | near))
        def _():
            z_pass(0, 0)

    def z_ahead(k):
        @pl.when(end & (k < last))
        def _():
            p = piece(k)
            for h in range(2):
                z_level(p, h, h == 0)
                z_copy(p, h).start()

    def z_finish():
        for h in range(2):
            z_level(z, h, h == 0)

            @pl.when(z > 0)
            def _():
                z_add(z, z, h)

            @pl.when(z < last)
            def _():
                z_add(z, n_z, h)

        for copy in z_first_copies():
            copy.start()

    def z_relay():
        for copy in z_first_copies():
            copy.wait_recv()
        for j in range(2):
            levz[intra, j, lo, z_part(0)] = levz[intra, j, lo, z_part(0)] + zfirst[0, j]
            levz[intra, hi, j, z_part(1)] = levz[intra, hi, j, z_part(1)] + zfirst[1, j]
        for copy in z_second_copies():
            copy.start()

    def lead_third(s):
        second_sum(0, s, True)

        @pl.when(end)
        def _():
            agg_copy(s).start()

        @pl.when(jnp.logical_not(end | near))
        def _():
            third_copy(piece(0), z, s, True).start()

    def near_third(k, s):
        @pl.when(near & (k == 2))
        def _():
            p = piece(0)
            i, r = p * CORES + core, rows_of(s, True)
            agg_copy(s).wait_recv()
            for h in range(2):
                lev[i, hi, lo, h, r] = lev[i, hi, lo, h, r] + agg[h, r]
            third_copy(p, z, s, True).start()

    def advance(k, is_first=False, is_last=False):
        for s in range(SUBS):
            with scope("G%d" % s):
                if not is_last:
                    level_piece(k + 1, s)
                    z_ahead(1 + k * SUBS + s)
                if not (is_first or is_last):
                    z_inner(k, s)
                with scope("Gf"):
                    first_sum(k, s)
                if is_first:
                    with scope("Gz"):
                        z_inner(k, s)
                if is_last:
                    with scope("Gz"):
                        if s == 0:
                            z_finish()
                        else:
                            z_relay()
                with scope("Gs"):
                    if is_first:
                        lead_third(s)
                        if s == 0:
                            z_ahead(2)
                    elif not is_last:
                        near_third(k, s)
                    if s == 0 and not is_first:
                        second_sum(k - 1, 1)
                        third_copy(piece(k - 1), z, 1).start()
                    elif s == 1:
                        second_sum(k, 0)
                        if not is_last:
                            third_copy(piece(k), z, 0).start()

    def middle(k, carry):
        advance(k)
        return carry

    with scope("F0"):
        level_piece(0, 1, True)
        z_lead()
        level_piece(1, 0)
        z_ahead(1)
        with scope("Fr"):
            raw_piece()
        level_piece(1, 1)
    with scope("F1"):
        with scope("Fz"):
            z_inner(0, 1)
        first_sum(0, 1, True)
    advance(1, is_first=True)
    lax.fori_loop(2, last, middle, 0)
    advance(last, is_last=True)
    with scope("K_last"):
        second_sum(last, 1)

    def from_plane(step, carry):
        other = lax.rem(z + step, n_z)

        def take(lead):
            for s in range(SUBS):
                r = rows_of(s, lead)
                third_copy(other, other, s, lead).wait_recv()
                for h in range(2):
                    lev[intra, hi, lo, h, r] = lev[intra, hi, lo, h, r] + third[other, h, r]

        lead = ((z == last) & (other < n_z // 2)) | ((z == 0) & (other >= n_z // 2))
        agged = jnp.abs(other - z) == last
        pl.when(lead & jnp.logical_not(agged))(lambda: take(True))
        pl.when(jnp.logical_not(lead | agged))(lambda: take(False))

        return carry

    with scope("L_third"):
        lax.fori_loop(1, n_z, from_plane, 0)
        for h in range(2):
            sum_ref[h * half : (h + 1) * half] = lev[intra, hi, lo, h]
    with scope("M_zlast"):
        for copy in z_second_copies():
            copy.wait_recv()
        for h in range(2):
            sum_ref[2 * half + h * zh : 2 * half + (h + 1) * zh] = (
                levz[intra, hi, lo, z_part(h)] + zsecond[h]
            )

    def finish(k, carry):
        p = piece(k)
        pair_copy(p).wait_send()
        pairz_copy(p).wait_send()

        @pl.when(k > 0)
        def _():
            for s in range(SUBS):
                for copy in first_copies(p, s) + second_copies(p, s):
                    copy.wait_send()

        @pl.when(k < last)
        def _():
            z_copy(p, 1).wait_send()

        @pl.when((k < last) & jnp.logical_not(end & (k == 0)))
        def _():
            z_copy(p, 0).wait_send()

        @pl.when((k == 0) & jnp.logical_not(end))
        def _():
            for s in range(SUBS):
                third_copy(p, z, s, True).wait_send()

        @pl.when((k > 0) & (k < last))
        def _():
            for s in range(SUBS):
                third_copy(p, z, s).wait_send()

        return carry

    with scope("N_finish"):
        all_peaks().wait_send()
        for flip in range(2):
            for copy in raw_copies(flip):
                copy.wait_send()
        p = piece(0)
        for copy in first_copies(p, 1, True) + second_copies(p, 0, True) + second_copies(p, 1, True):
            copy.wait_send()

        @pl.when(end)
        def _():
            for flip in range(2):
                zraw_copy(flip).wait_send()
            for s in range(SUBS):
                agg_copy(s).wait_send()

        lax.fori_loop(0, n_z, finish, 0)
        for copy in z_first_copies() + z_second_copies():
            copy.wait_send()


def adam_kernel(
    sum_ref, aux_ref, sign_ref, weight_ref, first_ref, second_ref,
    new_weight_ref, new_first_ref, new_second_ref, weight_buf, first_buf, second_buf, sems,
):
    owned = sum_ref.shape[0]
    table = parity_sign()
    table = jnp.concatenate([table * 64.0, table], axis=0).astype(jnp.bfloat16)
    signs = sign_ref[...]
    first_unbias, second_unbias = aux_ref[0:1], aux_ref[1:2]
    rows = owned // CHUNKS
    copies = []
    for c in range(CHUNKS):
        r = slice(c * rows, (c + 1) * rows)
        summed = sum_ref[r]
        high = jnp.floor(summed * (1.0 / 64.0))
        low = summed - high * 64.0
        both = jnp.concatenate([high, low], axis=1).astype(jnp.bfloat16)
        back = jnp.dot(both, table, preferred_element_type=jnp.float32)
        grad = (back.reshape(rows // SIGN_ROWS, SIGN_ROWS, BLOCK) * signs[None]).reshape(rows, BLOCK)
        new_first = 0.9 * first_ref[r] + 0.1 * grad
        new_second = 0.95 * second_ref[r] + 0.05 * grad * grad
        first_buf[r] = new_first
        second_buf[r] = new_second
        weights = weight_ref[r]
        update = (new_first * first_unbias) / (jnp.sqrt(new_second * second_unbias) + 1e-08)
        weight_buf[r] = weights - 0.2 * (update + 0.1 * weights)
        for n, (src, dst) in enumerate((
            (first_buf, new_first_ref), (second_buf, new_second_ref), (weight_buf, new_weight_ref),
        )):
            copy = pltpu.make_async_copy(src.at[r], dst.at[r], sems.at[n, c])
            copy.start()
            copies.append(copy)
    for copy in copies:
        copy.wait()


def shards(gradients, sign_table, loss_scale, step_count, weights, first_moment, second_moment):
    n_node, n_intra = lax.axis_size("node"), lax.axis_size("intra")
    n_z = n_intra // CORES
    n_dev = n_node * n_intra
    local = gradients.reshape(gradients.shape[2:])
    rows, columns = local.shape
    owned = weights.shape[0]
    z_rows, half = plan_rows(owned)
    zh = z_rows // 2
    n_hi = n_node // 2
    anywhere = pl.BlockSpec(memory_space=pl.ANY)
    smem = pl.BlockSpec(memory_space=pltpu.SMEM)
    hbm = functools.partial(pltpu.with_memory_space_constraint, memory_space=pltpu.HBM)
    vmem = pl.BlockSpec(memory_space=pltpu.VMEM)
    dma = pltpu.SemaphoreType.DMA
    f32 = jnp.float32
    slots = min(SLOTS, n_intra)
    buffers = [
        ((slots, owned, columns), jnp.bfloat16),
        ((SIGN_ROWS, columns), jnp.int32),
        ((SIGN_ROWS, columns), jnp.bfloat16),
        ((WIDE, WIDE), jnp.bfloat16),
    ]
    large = [
        ((n_intra, n_hi, 2, 2, half, BLOCK), f32),
        ((n_intra, n_hi, 2, z_rows, BLOCK), f32),
        ((n_z, n_hi, 2, 2, half, BLOCK), f32),
        ((n_z, n_hi, 2, z_rows, BLOCK), f32),
        ((2, 2, 2, half * 7 // 10 // 8 * 8, BLOCK), f32),
        ((2, n_hi, 2, zh, BLOCK), f32),
        ((n_z, 2, 2, half, BLOCK), f32),
        ((n_z, 2, half, BLOCK), f32),
        ((n_z, 2, half, BLOCK), f32),
        ((2, half, BLOCK), f32),
        ((n_z + 1, n_hi, 2, z_rows, BLOCK), f32),
        ((2, 2, zh, BLOCK), f32),
        ((2, zh, BLOCK), f32),
        ((n_dev, 1, BLOCK), f32),
    ]
    held = sum(math.prod(shape) * jnp.dtype(kind).itemsize for shape, kind in buffers + large)
    shape = (owned, BLOCK)
    outs = pl.pallas_call(
        functools.partial(reduce_kernel, n_node, n_intra),
        out_shape=(
            pltpu.VMEM(shape, f32), pltpu.VMEM((8, BLOCK), f32), pltpu.VMEM((SIGN_ROWS, BLOCK), f32),
            pltpu.VMEM(shape, f32), pltpu.VMEM(shape, f32), pltpu.VMEM(shape, f32),
        ),
        in_specs=[anywhere] * 2 + [smem] * 2 + [anywhere] * 3,
        out_specs=(vmem,) * 6,
        scratch_shapes=[pltpu.VMEM(*b) for b in buffers]
        + [pltpu.VMEM(*b) for b in large]
        + [
            dma((slots,)), dma((4,)),
            dma((n_z,)), dma((n_z,)), dma((n_z,)), dma((n_z,)),
            dma((2, 2)), dma((2, 2)), dma((2,)), dma((2,)),
            dma((2, n_z * SUBS)), dma((2, n_z * SUBS)),
            dma((2, n_z * SUBS)), dma((2, n_z * SUBS)),
            dma((n_z * SUBS,)), dma((n_z * SUBS,)),
            dma((SUBS,)), dma((SUBS,)),
            dma((n_z * 2,)), dma((n_z * 2 + 2,)),
            dma((2,)), dma((2,)), dma((2,)), dma((2,)),
            dma, dma,
        ],
        compiler_params=pltpu.CompilerParams(
            collective_id=0, has_side_effects=True, vmem_limit_bytes=held + (6 << 20)
        ),
    )(*(hbm(x) for x in (local, sign_table)), loss_scale, step_count,
      *(hbm(x) for x in (weights, first_moment, second_moment)))
    out = jax.ShapeDtypeStruct(shape, f32)
    return pl.pallas_call(
        adam_kernel,
        out_shape=(out, out, out),
        in_specs=[vmem] * 6,
        out_specs=(anywhere,) * 3,
        scratch_shapes=[pltpu.VMEM(shape, f32)] * 3 + [dma((3, CHUNKS))],
        compiler_params=pltpu.CompilerParams(vmem_limit_bytes=4 << 20),
    )(*outs)


def solution(mesh):
    own = P("intra", "node")
    return jax.shard_map(
        shards,
        mesh=mesh,
        in_specs=(P("node", "intra", None, None), P(), P(), P(), own, own, own),
        out_specs=(own, own, own),
        check_vma=False,
    )
```

```python
import contextlib
import functools
import math

import jax
import jax.numpy as jnp
from jax import lax
from jax.experimental import pallas as pl
from jax.experimental.pallas import tpu as pltpu
from jax.sharding import PartitionSpec as P

BLOCK = 128
WIDE = 2 * BLOCK
SIGN_ROWS = 64
CORES = 2
SLOTS = 8
SUBS = 2
CHUNKS = 3
ROOT = 1.0 / math.sqrt(BLOCK)
MESH = pl.DeviceIdType.MESH


def scope(name):
    return contextlib.nullcontext()


def parity_sign():
    shape = (BLOCK, BLOCK)
    parity = common = lax.broadcasted_iota(jnp.int32, shape, 0) & lax.broadcasted_iota(
        jnp.int32, shape, 1
    )
    for bit_index in range(1, BLOCK.bit_length() - 1):
        parity = parity ^ (common >> bit_index)
    return (1 - 2 * (parity & 1)).astype(jnp.float32)


def plan_rows(owned):
    z_rows = owned // 4 // 16 * 16
    return z_rows, (owned - z_rows) // 2


def reduce_kernel(
    n_node, n_intra, grad_ref, sign_ref, scale_ref, step_ref, weight_ref, first_ref, second_ref,
    sum_ref, aux_ref, sign_out, weight_out, first_out, second_out,
    stage, sign_tab, sign_bf, table_bf, lev, levz, pair, pairz, raw, zraw, first, second, third, agg,
    zin, zfirst, zsecond, peaks,
    load_sem, side_sem, pair_send, pair_recv, pairz_send, pairz_recv, raw_send, raw_recv,
    zraw_send, zraw_recv, first_send, first_recv, second_send, second_recv, third_send, third_recv,
    agg_send, agg_recv, zin_send, zin_recv, zfirst_send, zfirst_recv, zsecond_send, zsecond_recv,
    peak_send, peak_recv,
):
    n_z = n_intra // CORES
    last = n_z - 1
    n_dev = n_node * n_intra
    owned = sum_ref.shape[0]
    z_rows, half = plan_rows(owned)
    zh = z_rows // 2
    cut = (half // SUBS + 7) // 8 * 8
    spans = ((0, cut), (cut, half - cut))
    raw_rows = half * 8 // 10 // 8 * 8
    raw_spans = ((0, raw_rows), (raw_rows, half - raw_rows))
    node, intra = lax.axis_index("node"), lax.axis_index("intra")
    z, core = intra // CORES, intra % CORES
    hi, lo = node // 2, node % 2
    me = node * n_intra + intra
    end = (z == 0) | (z == last)
    near = (z == 1) | (z == last - 1)
    inward = jnp.where(z == 0, 1, last - 1)

    def at(node_index, z_index, core_index):
        return (node_index, z_index * CORES + core_index)

    def send(src, dst, send_sem, recv_sem, device):
        return pltpu.make_async_remote_copy(
            src_ref=src, dst_ref=dst, send_sem=send_sem, recv_sem=recv_sem,
            device_id=device, device_id_type=MESH,
        )

    def piece(k):
        lower = jnp.where(k < last - z, last - k, k - (last - z))
        upper = jnp.where(k < z, k, last - (k - z))
        return jnp.where(z < n_z // 2, lower, upper)

    def block_at(q):
        return piece(q // CORES) * CORES + jnp.where(q % CORES == 0, core, 1 - core)

    def load(q):
        slot = lax.rem(q, SLOTS)
        return pltpu.make_async_copy(
            grad_ref.at[pl.ds(block_at(q) * owned, owned)], stage.at[slot], load_sem.at[slot]
        )

    sides = [
        pltpu.make_async_copy(src, dst, side_sem.at[n])
        for n, (src, dst) in enumerate((
            (sign_ref, sign_tab), (weight_ref, weight_out), (first_ref, first_out), (second_ref, second_out),
        ))
    ]
    sides[0].start()
    for q in range(CORES):
        load(q).start()

    barrier = pltpu.get_barrier_semaphore()

    def everyone():
        for k in range(n_z):
            p = piece(k)
            for turn in range(n_node):
                other = lax.rem(node + turn, n_node)
                for flip in range(CORES):
                    if (k, turn, flip) != (last, 0, 0):
                        yield at(other, p, core if flip == 0 else 1 - core)

    for device in everyone():
        pl.semaphore_signal(barrier, inc=1, device_id=device, device_id_type=MESH)
    for q in range(CORES, min(SLOTS, n_intra)):
        load(q).start()
    for copy in sides[1:]:
        copy.start()
    table = parity_sign().astype(jnp.bfloat16)
    for a in range(2):
        for b in range(2):
            table_bf[a * BLOCK : (a + 1) * BLOCK, b * BLOCK : (b + 1) * BLOCK] = (
                table if a == b else jnp.zeros_like(table)
            )
    with scope("Asign"):
        sides[0].wait()
        sign_bf[...] = sign_tab[...].astype(jnp.float32).astype(jnp.bfloat16)

    def rotate(m, most):
        for q in range(CORES):
            load(m * CORES + q).wait()
        p = piece(m)
        blocks = [p * CORES + core, p * CORES + 1 - core]
        both_blocks = stage[pl.ds(lax.rem(m * CORES, SLOTS), CORES)].reshape(CORES * owned, -1)
        for w in range(n_node // 2):
            cols = slice(w * WIDE, (w + 1) * WIDE)
            part = both_blocks[:, cols].reshape(CORES * owned // SIGN_ROWS, SIGN_ROWS, WIDE)
            signed = (part * sign_bf[:, cols][None]).reshape(CORES * owned, WIDE)
            both = jnp.dot(signed, table_bf[...], preferred_element_type=jnp.float32)
            for c in range(CORES):
                for v in range(2):
                    spun = both[c * owned : (c + 1) * owned, v * BLOCK : (v + 1) * BLOCK]
                    for h in range(2):
                        lev[blocks[c], w, v, h] = spun[h * half : (h + 1) * half]
                    levz[blocks[c], w, v] = spun[2 * half :]
                    most = jnp.maximum(
                        most, jnp.max(jnp.abs(spun).reshape(owned // 8, 8, BLOCK), axis=0)
                    )
        for q in range(CORES):

            @pl.when(m * CORES + q + SLOTS < n_intra)
            def _():
                load(m * CORES + q + SLOTS).start()

        return most

    lo_peer = hi * 2 + 1 - lo
    hi_peer = (1 - hi) * 2 + lo

    def pair_copy(p):
        other = p * CORES + 1 - core
        return send(
            lev.at[other], pair.at[p], pair_send.at[p], pair_recv.at[p], at(node, z, 1 - core)
        )

    def pairz_copy(p):
        other = p * CORES + 1 - core
        return send(
            levz.at[other], pairz.at[p], pairz_send.at[p], pairz_recv.at[p], at(node, z, 1 - core)
        )

    def raw_copies(flip):
        target = core if flip == 0 else 1 - core
        i, r = piece(0) * CORES + target, pl.ds(0, raw_rows)
        return [
            send(
                src, raw.at[flip, h], raw_send.at[flip, h], raw_recv.at[flip, h],
                at(peer, z, target),
            )
            for h, src, peer in (
                (0, lev.at[i, :, 1 - lo, 0, r], lo_peer),
                (1, lev.at[i, 1 - hi, :, 1, r], hi_peer),
            )
        ]

    def zraw_copy(flip):
        target = core if flip == 0 else 1 - core
        return send(
            levz.at[piece(0) * CORES + target, :, :, z_part(0)], zraw.at[flip], zraw_send.at[flip], zraw_recv.at[flip],
            at(node, inward, target),
        )

    def rows_of(s, lead=False):
        return pl.ds(*(raw_spans if lead else spans)[s])

    def first_copies(p, s, lead=False):
        i, r = p * CORES + core, rows_of(s, lead)
        return [
            send(
                src, first.at[p, h, :, r], first_send.at[h, p * SUBS + s],
                first_recv.at[h, p * SUBS + s], at(peer, z, core),
            )
            for h, src, peer in (
                (0, lev.at[i, :, 1 - lo, 0, r], lo_peer),
                (1, lev.at[i, 1 - hi, :, 1, r], hi_peer),
            )
        ]

    def second_copies(p, s, lead=False):
        i, r = p * CORES + core, rows_of(s, lead)
        return [
            send(
                src, second.at[p, h, r], second_send.at[h, p * SUBS + s],
                second_recv.at[h, p * SUBS + s], at(peer, z, core),
            )
            for h, src, peer in (
                (0, lev.at[i, 1 - hi, lo, 0, r], hi_peer),
                (1, lev.at[i, hi, 1 - lo, 1, r], lo_peer),
            )
        ]

    def third_copy(p, slot, s, lead=False):
        r = rows_of(s, lead)
        return send(
            lev.at[p * CORES + core, hi, lo, :, r], third.at[slot, :, r],
            third_send.at[p * SUBS + s], third_recv.at[slot * SUBS + s], at(node, p, core),
        )

    def agg_copy(k, s, lead=False):
        r = rows_of(s, lead)
        return send(
            lev.at[piece(k) * CORES + core, hi, lo, :, r], agg.at[k, :, r],
            agg_send.at[k * SUBS + s], agg_recv.at[k * SUBS + s], at(node, inward, core),
        )

    def z_part(h):
        return pl.ds(h * zh, zh)

    def z_copy(p, h):
        onward = jnp.where(p > z, z + 1, z - 1)
        slot = jnp.where((p < z) & (p == onward), n_z, p)
        return send(
            levz.at[p * CORES + core, :, :, z_part(h)], zin.at[slot, :, :, z_part(h)],
            zin_send.at[p * 2 + h], zin_recv.at[slot * 2 + h], at(node, onward, core),
        )

    def z_arrived(slot, h):
        send(
            levz.at[core, :, :, z_part(h)], zin.at[slot, :, :, z_part(h)],
            zin_send.at[0], zin_recv.at[slot * 2 + h], at(node, inward, core),
        ).wait_recv()

    def z_first_copies():
        return [
            send(src, zfirst.at[h], zfirst_send.at[h], zfirst_recv.at[h], at(peer, z, core))
            for h, src, peer in (
                (0, levz.at[intra, :, 1 - lo, z_part(0)], lo_peer),
                (1, levz.at[intra, 1 - hi, :, z_part(1)], hi_peer),
            )
        ]

    def z_second_copies():
        return [
            send(src, zsecond.at[h], zsecond_send.at[h], zsecond_recv.at[h], at(peer, z, core))
            for h, src, peer in (
                (0, levz.at[intra, 1 - hi, lo, z_part(0)], hi_peer),
                (1, levz.at[intra, hi, 1 - lo, z_part(1)], lo_peer),
            )
        ]

    def peak_copy(device):
        return send(peaks.at[me], peaks.at[me], peak_send, peak_recv, device)

    def all_peaks():
        every = peaks.at[pl.ds(0, n_dev - 1)]
        return send(every, every, peak_send, peak_recv, at(node, z, 1 - core))

    with scope("A_rotate"):
        most = lax.fori_loop(0, n_z, rotate, jnp.zeros((8, BLOCK), jnp.float32))
        peaks[me] = jnp.max(most, axis=0, keepdims=True)
    with scope("B_barrier"):
        pl.semaphore_wait(barrier, n_dev - 1)

    with scope("C_issue"):
        for device in everyone():
            peak_copy(device).start()
        for flip in range(2):
            for copy in raw_copies(flip):
                copy.start()

        @pl.when(end)
        def _():
            for flip in range(2):
                zraw_copy(flip).start()

        def share(k, carry):
            pair_copy(piece(k)).start()
            pairz_copy(piece(k)).start()
            return carry

        lax.fori_loop(0, n_z, share, 0)

    with scope("D_sides"):
        for copy in sides[1:]:
            copy.wait()
        ones = jnp.ones((1, BLOCK), jnp.float32)
        steps = ones * step_ref[0].astype(jnp.float32)
        aux_ref[0:1] = 1.0 / (1.0 - jnp.exp(steps * math.log(0.9)))
        aux_ref[1:2] = 1.0 / (1.0 - jnp.exp(steps * math.log(0.95)))

    with scope("E_peaks"):
        all_peaks().wait_recv()
        tops = jnp.max(peaks[...], axis=0)
        top_value = jnp.max(tops, axis=1, keepdims=True) * ROOT
        level_scale = 127.0 / top_value
        factor = (ones * top_value) / (ones * (127.0 * float(n_dev) * scale_ref[0]))
        column = pl.multiple_of(node * BLOCK, BLOCK)
        sign_out[...] = sign_tab[:, pl.ds(column, BLOCK)].astype(jnp.float32) * (factor * ROOT)

    def level(value):
        return jnp.floor((value * ROOT) * level_scale + 0.5)

    def level_piece(k, s, lead=False):
        p = piece(k)
        i, r = p * CORES + core, rows_of(s, lead)
        if lead or (s == 0):
            pair_copy(p).wait_recv()
        for j in range(n_node):
            for h in range(2):
                spot = (j // 2, j % 2, h, r)
                lev[(i,) + spot] = level(lev[(i,) + spot]) + level(pair[(p,) + spot])
        for copy in first_copies(p, s, lead):
            copy.start()

    def first_sum(k, s, lead=False):
        p = piece(k)
        i, r = p * CORES + core, rows_of(s, lead)
        for copy in first_copies(p, s, lead):
            copy.wait_recv()
        for j in range(2):
            lev[i, j, lo, 0, r] = lev[i, j, lo, 0, r] + first[p, 0, j, r]
            lev[i, hi, j, 1, r] = lev[i, hi, j, 1, r] + first[p, 1, j, r]
        for copy in second_copies(p, s, lead):
            copy.start()

    def second_sum(k, s, lead=False):
        p = piece(k)
        i, r = p * CORES + core, rows_of(s, lead)
        for copy in second_copies(p, s, lead):
            copy.wait_recv()
        for h in range(2):
            lev[i, hi, lo, h, r] = lev[i, hi, lo, h, r] + second[p, h, r]

    def raw_piece():
        p = piece(0)
        i, r = p * CORES + core, rows_of(0, True)
        for flip in range(2):
            for copy in raw_copies(flip):
                copy.wait_recv()

        def kept(h, j, spot):
            lev[(i,) + spot] = (
                level(lev[(i,) + spot]) + level(pair[(p,) + spot])
                + level(raw[0, h, j]) + level(raw[1, h, j])
            )

        for j in range(2):
            kept(0, j, (j, lo, 0, r))
            kept(1, j, (hi, j, 1, r))
        for copy in second_copies(p, 0, True):
            copy.start()

    def z_level(p, h, wait):
        i, r = p * CORES + core, z_part(h)
        if wait:
            pairz_copy(p).wait_recv()
        for j in range(n_node):
            spot = (j // 2, j % 2, r)
            levz[(i,) + spot] = level(levz[(i,) + spot]) + level(pairz[(p,) + spot])

    def z_add(p, slot, h):
        i, r = p * CORES + core, z_part(h)
        z_arrived(slot, h)
        for j in range(n_node):
            spot = (j // 2, j % 2, r)
            levz[(i,) + spot] = levz[(i,) + spot] + zin[(slot,) + spot]

    def z_pass(k, h):
        p = piece(k)
        z_level(p, h, h == 0)
        z_add(p, p, h)
        z_copy(p, h).start()

    def z_inner(k, h):
        @pl.when(jnp.logical_not(end))
        def _():
            z_pass(k, h)

    def z_lead():
        @pl.when(end)
        def _():
            z_level(piece(0), 1, True)
            z_copy(piece(0), 1).start()

        @pl.when(near)
        def _():
            p = piece(0)
            i, r = p * CORES + core, z_part(0)
            z_level(p, 0, True)
            for flip in range(2):
                zraw_copy(flip).wait_recv()
            for j in range(n_node):
                spot = (j // 2, j % 2)
                levz[(i,) + spot + (r,)] = (
                    levz[(i,) + spot + (r,)]
                    + level(zraw[(0,) + spot]) + level(zraw[(1,) + spot])
                )
            z_copy(p, 0).start()

        @pl.when(jnp.logical_not(end | near))
        def _():
            z_pass(0, 0)

    def z_ahead(k, h):
        @pl.when(end & (k < last))
        def _():
            p = piece(k)
            z_level(p, h, h == 0)
            z_copy(p, h).start()

    def z_finish():
        for h in range(2):
            z_level(z, h, h == 0)

            @pl.when(z > 0)
            def _():
                z_add(z, z, h)

            @pl.when(z < last)
            def _():
                z_add(z, n_z, h)

        for copy in z_first_copies():
            copy.start()

    def z_relay():
        for copy in z_first_copies():
            copy.wait_recv()
        for j in range(2):
            levz[intra, j, lo, z_part(0)] = levz[intra, j, lo, z_part(0)] + zfirst[0, j]
            levz[intra, hi, j, z_part(1)] = levz[intra, hi, j, z_part(1)] + zfirst[1, j]
        for copy in z_second_copies():
            copy.start()

    def give_third(k, s, lead=False):
        p = piece(k)
        second_sum(k, s, lead)
        via = k <= last - 2

        @pl.when(end & via)
        def _():
            agg_copy(k, s, lead).start()

        @pl.when(jnp.logical_not((end | near) & via))
        def _():
            third_copy(p, z, s, lead).start()

    def near_third(k, s, lead=False):
        @pl.when(near)
        def _():
            p = piece(k)
            i, r = p * CORES + core, rows_of(s, lead)
            agg_copy(k, s, lead).wait_recv()
            for h in range(2):
                lev[i, hi, lo, h, r] = lev[i, hi, lo, h, r] + agg[k, h, r]
            third_copy(p, z, s, lead).start()

    def begin():
        with scope("G0"):
            first_sum(1, 0)
            level_piece(2, 1)
            with scope("Gz"):
                z_inner(1, 0)
                z_inner(2, 0)
            z_ahead(2, 0)
            with scope("Gs"):
                give_third(0, 0, True)
            z_ahead(2, 1)
        with scope("G1"):
            first_sum(1, 1)
            level_piece(3, 0)
            with scope("Gz"):
                z_inner(1, 1)
                z_inner(2, 1)
            with scope("Gn"):
                near_third(0, 0, True)
            with scope("Gs"):
                give_third(0, 1, True)
            with scope("Gs"):
                give_third(1, 0)

    def middle(k, carry):
        with scope("M0"):
            first_sum(k, 0)
        with scope("M1"):
            first_sum(k, 1)
        level_piece(k + 1, 1)
        pl.when(k + 2 <= last)(lambda: level_piece(k + 2, 0))
        for h in range(2):
            z_ahead(k + 1, h)
            pl.when(k + 1 < last)(lambda: z_inner(k + 1, h))
        with scope("M2"):
            give_third(k - 1, 1)
        with scope("Mz"):
            pl.when(k == last - 1)(z_finish)
        with scope("M3"):

            @pl.when(k == 2)
            def _():
                near_third(0, 1, True)

            @pl.when(k > 2)
            def _():
                for s in range(SUBS):
                    near_third(k - 2, s)

        with scope("M4"):
            give_third(k, 0)
        return carry

    with scope("F0"):
        level_piece(0, 1, True)
        z_lead()
        level_piece(1, 0)
        for h in range(2):
            z_ahead(1, h)
        with scope("Fr"):
            raw_piece()
        level_piece(1, 1)
    with scope("F1"):
        with scope("Fz"):
            z_inner(0, 1)
        first_sum(0, 1, True)
        level_piece(2, 0)
    begin()
    lax.fori_loop(2, last, middle, 0)
    with scope("H0"):
        first_sum(last, 0)
    with scope("H1"):
        give_third(last - 1, 1)
    with scope("H2"):
        for s in range(SUBS):
            near_third(last - 2, s)
    with scope("H3"):
        first_sum(last, 1)
    with scope("H4"):
        z_relay()
    with scope("K0"):
        second_sum(last, 0)
    with scope("K1"):
        second_sum(last, 1)

    def from_plane(step, carry):
        other = lax.rem(z + step, n_z)

        def take(lead):
            for s in range(SUBS):
                r = rows_of(s, lead)
                third_copy(other, other, s, lead).wait_recv()
                for h in range(2):
                    lev[intra, hi, lo, h, r] = lev[intra, hi, lo, h, r] + third[other, h, r]

        lead = ((z == last) & (other < n_z // 2)) | ((z == 0) & (other >= n_z // 2))
        agged = ((other == 0) | (other == last)) & (jnp.abs(other - z) > 1)
        pl.when(lead & jnp.logical_not(agged))(lambda: take(True))
        pl.when(jnp.logical_not(lead | agged))(lambda: take(False))

        return carry

    with scope("L_third"):
        lax.fori_loop(1, n_z, from_plane, 0)
        for h in range(2):
            sum_ref[h * half : (h + 1) * half] = lev[intra, hi, lo, h]
    with scope("M_zlast"):
        for copy in z_second_copies():
            copy.wait_recv()
        for h in range(2):
            sum_ref[2 * half + h * zh : 2 * half + (h + 1) * zh] = (
                levz[intra, hi, lo, z_part(h)] + zsecond[h]
            )

    def finish(k, carry):
        p = piece(k)
        pair_copy(p).wait_send()
        pairz_copy(p).wait_send()

        @pl.when(k > 0)
        def _():
            for s in range(SUBS):
                for copy in first_copies(p, s) + second_copies(p, s):
                    copy.wait_send()

        @pl.when(k < last)
        def _():
            z_copy(p, 1).wait_send()

        @pl.when((k < last) & jnp.logical_not(end & (k == 0)))
        def _():
            z_copy(p, 0).wait_send()

        def gave(lead):
            via = end & (k <= last - 2)
            for s in range(SUBS):
                pl.when(via)(lambda: agg_copy(k, s, lead).wait_send())
                pl.when(jnp.logical_not(via))(lambda: third_copy(p, z, s, lead).wait_send())

        pl.when(k == 0)(lambda: gave(True))
        pl.when((k > 0) & (k < last))(lambda: gave(False))

        return carry

    with scope("N_finish"):
        all_peaks().wait_send()
        for flip in range(2):
            for copy in raw_copies(flip):
                copy.wait_send()
        p = piece(0)
        for copy in first_copies(p, 1, True) + second_copies(p, 0, True) + second_copies(p, 1, True):
            copy.wait_send()

        @pl.when(end)
        def _():
            for flip in range(2):
                zraw_copy(flip).wait_send()

        lax.fori_loop(0, n_z, finish, 0)
        for copy in z_first_copies() + z_second_copies():
            copy.wait_send()


def adam_kernel(
    sum_ref, aux_ref, sign_ref, weight_ref, first_ref, second_ref,
    new_weight_ref, new_first_ref, new_second_ref, weight_buf, first_buf, second_buf, sems,
):
    owned = sum_ref.shape[0]
    table = parity_sign()
    table = jnp.concatenate([table * 64.0, table], axis=0).astype(jnp.bfloat16)
    signs = sign_ref[...]
    first_unbias, second_unbias = aux_ref[0:1], aux_ref[1:2]
    rows = owned // CHUNKS
    copies = []
    for c in range(CHUNKS):
        r = slice(c * rows, (c + 1) * rows)
        summed = sum_ref[r]
        high = jnp.floor(summed * (1.0 / 64.0))
        low = summed - high * 64.0
        both = jnp.concatenate([high, low], axis=1).astype(jnp.bfloat16)
        back = jnp.dot(both, table, preferred_element_type=jnp.float32)
        grad = (back.reshape(rows // SIGN_ROWS, SIGN_ROWS, BLOCK) * signs[None]).reshape(rows, BLOCK)
        new_first = 0.9 * first_ref[r] + 0.1 * grad
        new_second = 0.95 * second_ref[r] + 0.05 * grad * grad
        first_buf[r] = new_first
        second_buf[r] = new_second
        weights = weight_ref[r]
        update = (new_first * first_unbias) / (jnp.sqrt(new_second * second_unbias) + 1e-08)
        weight_buf[r] = weights - 0.2 * (update + 0.1 * weights)
        for n, (src, dst) in enumerate((
            (first_buf, new_first_ref), (second_buf, new_second_ref), (weight_buf, new_weight_ref),
        )):
            copy = pltpu.make_async_copy(src.at[r], dst.at[r], sems.at[n, c])
            copy.start()
            copies.append(copy)
    for copy in copies:
        copy.wait()


def shards(gradients, sign_table, loss_scale, step_count, weights, first_moment, second_moment):
    n_node, n_intra = lax.axis_size("node"), lax.axis_size("intra")
    n_z = n_intra // CORES
    n_dev = n_node * n_intra
    local = gradients.reshape(gradients.shape[2:])
    rows, columns = local.shape
    owned = weights.shape[0]
    z_rows, half = plan_rows(owned)
    zh = z_rows // 2
    n_hi = n_node // 2
    anywhere = pl.BlockSpec(memory_space=pl.ANY)
    smem = pl.BlockSpec(memory_space=pltpu.SMEM)
    hbm = functools.partial(pltpu.with_memory_space_constraint, memory_space=pltpu.HBM)
    vmem = pl.BlockSpec(memory_space=pltpu.VMEM)
    dma = pltpu.SemaphoreType.DMA
    f32 = jnp.float32
    slots = min(SLOTS, n_intra)
    buffers = [
        ((slots, owned, columns), jnp.bfloat16),
        ((SIGN_ROWS, columns), jnp.int32),
        ((SIGN_ROWS, columns), jnp.bfloat16),
        ((WIDE, WIDE), jnp.bfloat16),
    ]
    large = [
        ((n_intra, n_hi, 2, 2, half, BLOCK), f32),
        ((n_intra, n_hi, 2, z_rows, BLOCK), f32),
        ((n_z, n_hi, 2, 2, half, BLOCK), f32),
        ((n_z, n_hi, 2, z_rows, BLOCK), f32),
        ((2, 2, 2, half * 8 // 10 // 8 * 8, BLOCK), f32),
        ((2, n_hi, 2, zh, BLOCK), f32),
        ((n_z, 2, 2, half, BLOCK), f32),
        ((n_z, 2, half, BLOCK), f32),
        ((n_z, 2, half, BLOCK), f32),
        ((n_z - 2, 2, half, BLOCK), f32),
        ((n_z + 1, n_hi, 2, z_rows, BLOCK), f32),
        ((2, 2, zh, BLOCK), f32),
        ((2, zh, BLOCK), f32),
        ((n_dev, 1, BLOCK), f32),
    ]
    held = sum(math.prod(shape) * jnp.dtype(kind).itemsize for shape, kind in buffers + large)
    shape = (owned, BLOCK)
    outs = pl.pallas_call(
        functools.partial(reduce_kernel, n_node, n_intra),
        out_shape=(
            pltpu.VMEM(shape, f32), pltpu.VMEM((8, BLOCK), f32), pltpu.VMEM((SIGN_ROWS, BLOCK), f32),
            pltpu.VMEM(shape, f32), pltpu.VMEM(shape, f32), pltpu.VMEM(shape, f32),
        ),
        in_specs=[anywhere] * 2 + [smem] * 2 + [anywhere] * 3,
        out_specs=(vmem,) * 6,
        scratch_shapes=[pltpu.VMEM(*b) for b in buffers]
        + [pltpu.VMEM(*b) for b in large]
        + [
            dma((slots,)), dma((4,)),
            dma((n_z,)), dma((n_z,)), dma((n_z,)), dma((n_z,)),
            dma((2, 2)), dma((2, 2)), dma((2,)), dma((2,)),
            dma((2, n_z * SUBS)), dma((2, n_z * SUBS)),
            dma((2, n_z * SUBS)), dma((2, n_z * SUBS)),
            dma((n_z * SUBS,)), dma((n_z * SUBS,)),
            dma(((n_z - 2) * SUBS,)), dma(((n_z - 2) * SUBS,)),
            dma((n_z * 2,)), dma((n_z * 2 + 2,)),
            dma((2,)), dma((2,)), dma((2,)), dma((2,)),
            dma, dma,
        ],
        compiler_params=pltpu.CompilerParams(
            collective_id=0, has_side_effects=True, vmem_limit_bytes=held + (6 << 20)
        ),
    )(*(hbm(x) for x in (local, sign_table)), loss_scale, step_count,
      *(hbm(x) for x in (weights, first_moment, second_moment)))
    out = jax.ShapeDtypeStruct(shape, f32)
    return pl.pallas_call(
        adam_kernel,
        out_shape=(out, out, out),
        in_specs=[vmem] * 6,
        out_specs=(anywhere,) * 3,
        scratch_shapes=[pltpu.VMEM(shape, f32)] * 3 + [dma((3, CHUNKS))],
        compiler_params=pltpu.CompilerParams(vmem_limit_bytes=4 << 20),
    )(*outs)


def solution(mesh):
    own = P("intra", "node")
    return jax.shard_map(
        shards,
        mesh=mesh,
        in_specs=(P("node", "intra", None, None), P(), P(), P(), own, own, own),
        out_specs=(own, own, own),
        check_vma=False,
    )
```

```python
import contextlib
import functools
import math

import jax
import jax.numpy as jnp
from jax import lax
from jax.experimental import pallas as pl
from jax.experimental.pallas import tpu as pltpu
from jax.sharding import PartitionSpec as P

BLOCK = 128
WIDE = 2 * BLOCK
SIGN_ROWS = 64
CORES = 2
SLOTS = 8
SUBS = 2
ROOT = 1.0 / math.sqrt(BLOCK)
MESH = pl.DeviceIdType.MESH


def scope(name):
    return contextlib.nullcontext()


def parity_sign():
    shape = (BLOCK, BLOCK)
    parity = common = lax.broadcasted_iota(jnp.int32, shape, 0) & lax.broadcasted_iota(
        jnp.int32, shape, 1
    )
    for bit_index in range(1, BLOCK.bit_length() - 1):
        parity = parity ^ (common >> bit_index)
    return (1 - 2 * (parity & 1)).astype(jnp.float32)


def plan_rows(owned):
    z_rows = owned // 4 // 16 * 16
    return z_rows, (owned - z_rows) // 2


def reduce_kernel(
    n_node, n_intra, grad_ref, sign_ref, scale_ref, step_ref, weight_ref, first_ref, second_ref,
    new_weight_ref, new_first_ref, new_second_ref,
    stage, sign_tab, sign_bf, table_bf, split_bf, sign_own, weight_in, first_in, second_in, lev, levz, pair, pairz, raw, zraw, first, second, third, agg,
    zin, zfirst, zsecond, peaks,
    load_sem, side_sem, pair_send, pair_recv, pairz_send, pairz_recv, raw_send, raw_recv,
    zraw_send, zraw_recv, first_send, first_recv, second_send, second_recv, third_send, third_recv,
    agg_send, agg_recv, zin_send, zin_recv, zfirst_send, zfirst_recv, zsecond_send, zsecond_recv,
    peak_send, peak_recv,
):
    n_z = n_intra // CORES
    last = n_z - 1
    n_dev = n_node * n_intra
    owned = new_weight_ref.shape[0]
    z_rows, half = plan_rows(owned)
    zh = z_rows // 2
    cut = (half // SUBS + 7) // 8 * 8
    spans = ((0, cut), (cut, half - cut))
    raw_rows = half * 8 // 10 // 8 * 8
    raw_spans = ((0, raw_rows), (raw_rows, half - raw_rows))
    node, intra = lax.axis_index("node"), lax.axis_index("intra")
    z, core = intra // CORES, intra % CORES
    hi, lo = node // 2, node % 2
    me = node * n_intra + intra
    end = (z == 0) | (z == last)
    near = (z == 1) | (z == last - 1)
    inward = jnp.where(z == 0, 1, last - 1)

    def at(node_index, z_index, core_index):
        return (node_index, z_index * CORES + core_index)

    def send(src, dst, send_sem, recv_sem, device):
        return pltpu.make_async_remote_copy(
            src_ref=src, dst_ref=dst, send_sem=send_sem, recv_sem=recv_sem,
            device_id=device, device_id_type=MESH,
        )

    def piece(k):
        lower = jnp.where(k < last - z, last - k, k - (last - z))
        upper = jnp.where(k < z, k, last - (k - z))
        return jnp.where(z < n_z // 2, lower, upper)

    def block_at(q):
        return piece(q // CORES) * CORES + jnp.where(q % CORES == 0, core, 1 - core)

    def load(q):
        slot = lax.rem(q, SLOTS)
        return pltpu.make_async_copy(
            grad_ref.at[pl.ds(block_at(q) * owned, owned)], stage.at[slot], load_sem.at[slot]
        )

    sides = [
        pltpu.make_async_copy(src, dst, side_sem.at[n])
        for n, (src, dst) in enumerate((
            (sign_ref, sign_tab), (weight_ref, weight_in), (first_ref, first_in), (second_ref, second_in),
        ))
    ]
    sides[0].start()
    for q in range(CORES):
        load(q).start()

    barrier = pltpu.get_barrier_semaphore()

    def everyone():
        for k in range(n_z):
            p = piece(k)
            for turn in range(n_node):
                other = lax.rem(node + turn, n_node)
                for flip in range(CORES):
                    if (k, turn, flip) != (last, 0, 0):
                        yield at(other, p, core if flip == 0 else 1 - core)

    for device in everyone():
        pl.semaphore_signal(barrier, inc=1, device_id=device, device_id_type=MESH)
    for q in range(CORES, min(SLOTS, n_intra)):
        load(q).start()
    for copy in sides[1:]:
        copy.start()
    table = parity_sign().astype(jnp.bfloat16)
    for a in range(2):
        for b in range(2):
            table_bf[a * BLOCK : (a + 1) * BLOCK, b * BLOCK : (b + 1) * BLOCK] = (
                table if a == b else jnp.zeros_like(table)
            )
    with scope("Asign"):
        sides[0].wait()
        sign_bf[...] = sign_tab[...].astype(jnp.float32).astype(jnp.bfloat16)

    def rotate(m, most):
        for q in range(CORES):
            load(m * CORES + q).wait()
        p = piece(m)
        blocks = [p * CORES + core, p * CORES + 1 - core]
        both_blocks = stage[pl.ds(lax.rem(m * CORES, SLOTS), CORES)].reshape(CORES * owned, -1)
        for w in range(n_node // 2):
            cols = slice(w * WIDE, (w + 1) * WIDE)
            part = both_blocks[:, cols].reshape(CORES * owned // SIGN_ROWS, SIGN_ROWS, WIDE)
            signed = (part * sign_bf[:, cols][None]).reshape(CORES * owned, WIDE)
            both = jnp.dot(signed, table_bf[...], preferred_element_type=jnp.float32)
            for c in range(CORES):
                for v in range(2):
                    spun = both[c * owned : (c + 1) * owned, v * BLOCK : (v + 1) * BLOCK]
                    for h in range(2):
                        lev[blocks[c], w, v, h] = spun[h * half : (h + 1) * half]
                    levz[blocks[c], w, v] = spun[2 * half :]
                    most = jnp.maximum(
                        most, jnp.max(jnp.abs(spun).reshape(owned // 8, 8, BLOCK), axis=0)
                    )
        for q in range(CORES):

            @pl.when(m * CORES + q + SLOTS < n_intra)
            def _():
                load(m * CORES + q + SLOTS).start()

        return most

    lo_peer = hi * 2 + 1 - lo
    hi_peer = (1 - hi) * 2 + lo

    def pair_copy(p):
        other = p * CORES + 1 - core
        return send(
            lev.at[other], pair.at[p], pair_send.at[p], pair_recv.at[p], at(node, z, 1 - core)
        )

    def pairz_copy(p):
        other = p * CORES + 1 - core
        return send(
            levz.at[other], pairz.at[p], pairz_send.at[p], pairz_recv.at[p], at(node, z, 1 - core)
        )

    def raw_copies(flip):
        target = core if flip == 0 else 1 - core
        i, r = piece(0) * CORES + target, pl.ds(0, raw_rows)
        return [
            send(
                src, raw.at[flip, h], raw_send.at[flip, h], raw_recv.at[flip, h],
                at(peer, z, target),
            )
            for h, src, peer in (
                (0, lev.at[i, :, 1 - lo, 0, r], lo_peer),
                (1, lev.at[i, 1 - hi, :, 1, r], hi_peer),
            )
        ]

    def zraw_copy(flip):
        target = core if flip == 0 else 1 - core
        return send(
            levz.at[piece(0) * CORES + target, :, :, z_part(0)], zraw.at[flip], zraw_send.at[flip], zraw_recv.at[flip],
            at(node, inward, target),
        )

    def rows_of(s, lead=False):
        return pl.ds(*(raw_spans if lead else spans)[s])

    def first_copies(p, s, lead=False):
        i, r = p * CORES + core, rows_of(s, lead)
        return [
            send(
                src, first.at[p, h, :, r], first_send.at[h, p * SUBS + s],
                first_recv.at[h, p * SUBS + s], at(peer, z, core),
            )
            for h, src, peer in (
                (0, lev.at[i, :, 1 - lo, 0, r], lo_peer),
                (1, lev.at[i, 1 - hi, :, 1, r], hi_peer),
            )
        ]

    def second_copies(p, s, lead=False):
        i, r = p * CORES + core, rows_of(s, lead)
        return [
            send(
                src, second.at[p, h, r], second_send.at[h, p * SUBS + s],
                second_recv.at[h, p * SUBS + s], at(peer, z, core),
            )
            for h, src, peer in (
                (0, lev.at[i, 1 - hi, lo, 0, r], hi_peer),
                (1, lev.at[i, hi, 1 - lo, 1, r], lo_peer),
            )
        ]

    def third_copy(p, slot, s, lead=False):
        r = rows_of(s, lead)
        return send(
            lev.at[p * CORES + core, hi, lo, :, r], third.at[slot, :, r],
            third_send.at[p * SUBS + s], third_recv.at[slot * SUBS + s], at(node, p, core),
        )

    def agg_copy(k, s, lead=False):
        r = rows_of(s, lead)
        return send(
            lev.at[piece(k) * CORES + core, hi, lo, :, r], agg.at[k, :, r],
            agg_send.at[k * SUBS + s], agg_recv.at[k * SUBS + s], at(node, inward, core),
        )

    def z_part(h):
        return pl.ds(h * zh, zh)

    def z_copy(p, h):
        onward = jnp.where(p > z, z + 1, z - 1)
        slot = jnp.where((p < z) & (p == onward), n_z, p)
        return send(
            levz.at[p * CORES + core, :, :, z_part(h)], zin.at[slot, :, :, z_part(h)],
            zin_send.at[p * 2 + h], zin_recv.at[slot * 2 + h], at(node, onward, core),
        )

    def z_arrived(slot, h):
        send(
            levz.at[core, :, :, z_part(h)], zin.at[slot, :, :, z_part(h)],
            zin_send.at[0], zin_recv.at[slot * 2 + h], at(node, inward, core),
        ).wait_recv()

    def z_first_copies():
        return [
            send(src, zfirst.at[h], zfirst_send.at[h], zfirst_recv.at[h], at(peer, z, core))
            for h, src, peer in (
                (0, levz.at[intra, :, 1 - lo, z_part(0)], lo_peer),
                (1, levz.at[intra, 1 - hi, :, z_part(1)], hi_peer),
            )
        ]

    def z_second_copies():
        return [
            send(src, zsecond.at[h], zsecond_send.at[h], zsecond_recv.at[h], at(peer, z, core))
            for h, src, peer in (
                (0, levz.at[intra, 1 - hi, lo, z_part(0)], hi_peer),
                (1, levz.at[intra, hi, 1 - lo, z_part(1)], lo_peer),
            )
        ]

    def peak_copy(device):
        return send(peaks.at[me], peaks.at[me], peak_send, peak_recv, device)

    def all_peaks():
        every = peaks.at[pl.ds(0, n_dev - 1)]
        return send(every, every, peak_send, peak_recv, at(node, z, 1 - core))

    with scope("A_rotate"):
        most = lax.fori_loop(0, n_z, rotate, jnp.zeros((8, BLOCK), jnp.float32))
        peaks[me] = jnp.max(most, axis=0, keepdims=True)
    with scope("B_barrier"):
        pl.semaphore_wait(barrier, n_dev - 1)

    with scope("C_issue"):
        for device in everyone():
            peak_copy(device).start()
        for flip in range(2):
            for copy in raw_copies(flip):
                copy.start()

        @pl.when(end)
        def _():
            for flip in range(2):
                zraw_copy(flip).start()

        def share(k, carry):
            pair_copy(piece(k)).start()
            pairz_copy(piece(k)).start()
            return carry

        lax.fori_loop(0, n_z, share, 0)

    with scope("D_sides"):
        for copy in sides[1:]:
            copy.wait()
        ones = jnp.ones((1, BLOCK), jnp.float32)
        steps = ones * step_ref[0].astype(jnp.float32)
        first_unbias = 1.0 / (1.0 - jnp.exp(steps * math.log(0.9)))
        second_unbias = 1.0 / (1.0 - jnp.exp(steps * math.log(0.95)))
        split_bf[0:BLOCK] = (parity_sign() * 64.0).astype(jnp.bfloat16)
        split_bf[BLOCK:] = parity_sign().astype(jnp.bfloat16)

    with scope("E_peaks"):
        all_peaks().wait_recv()
        tops = jnp.max(peaks[...], axis=0)
        top_value = jnp.max(tops, axis=1, keepdims=True) * ROOT
        level_scale = 127.0 / top_value

    def level(value):
        return jnp.floor((value * ROOT) * level_scale + 0.5)

    def level_piece(k, s, lead=False):
        p = piece(k)
        i, r = p * CORES + core, rows_of(s, lead)
        if lead or (s == 0):
            pair_copy(p).wait_recv()
        for j in range(n_node):
            for h in range(2):
                spot = (j // 2, j % 2, h, r)
                lev[(i,) + spot] = level(lev[(i,) + spot]) + level(pair[(p,) + spot])
        for copy in first_copies(p, s, lead):
            copy.start()

    def first_sum(k, s, lead=False):
        p = piece(k)
        i, r = p * CORES + core, rows_of(s, lead)
        for copy in first_copies(p, s, lead):
            copy.wait_recv()
        for j in range(2):
            lev[i, j, lo, 0, r] = lev[i, j, lo, 0, r] + first[p, 0, j, r]
            lev[i, hi, j, 1, r] = lev[i, hi, j, 1, r] + first[p, 1, j, r]
        for copy in second_copies(p, s, lead):
            copy.start()

    def second_sum(k, s, lead=False):
        p = piece(k)
        i, r = p * CORES + core, rows_of(s, lead)
        for copy in second_copies(p, s, lead):
            copy.wait_recv()
        for h in range(2):
            lev[i, hi, lo, h, r] = lev[i, hi, lo, h, r] + second[p, h, r]

    def raw_piece():
        p = piece(0)
        i, r = p * CORES + core, rows_of(0, True)
        for flip in range(2):
            for copy in raw_copies(flip):
                copy.wait_recv()

        def kept(h, j, spot):
            lev[(i,) + spot] = (
                level(lev[(i,) + spot]) + level(pair[(p,) + spot])
                + level(raw[0, h, j]) + level(raw[1, h, j])
            )

        for j in range(2):
            kept(0, j, (j, lo, 0, r))
            kept(1, j, (hi, j, 1, r))
        for copy in second_copies(p, 0, True):
            copy.start()

    def z_level(p, h, wait):
        i, r = p * CORES + core, z_part(h)
        if wait:
            pairz_copy(p).wait_recv()
        for j in range(n_node):
            spot = (j // 2, j % 2, r)
            levz[(i,) + spot] = level(levz[(i,) + spot]) + level(pairz[(p,) + spot])

    def z_add(p, slot, h):
        i, r = p * CORES + core, z_part(h)
        z_arrived(slot, h)
        for j in range(n_node):
            spot = (j // 2, j % 2, r)
            levz[(i,) + spot] = levz[(i,) + spot] + zin[(slot,) + spot]

    def z_pass(k, h):
        p = piece(k)
        z_level(p, h, h == 0)
        z_add(p, p, h)
        z_copy(p, h).start()

    def z_inner(k, h):
        @pl.when(jnp.logical_not(end))
        def _():
            z_pass(k, h)

    def z_lead():
        @pl.when(end)
        def _():
            z_level(piece(0), 1, True)
            z_copy(piece(0), 1).start()

        @pl.when(near)
        def _():
            p = piece(0)
            i, r = p * CORES + core, z_part(0)
            z_level(p, 0, True)
            for flip in range(2):
                zraw_copy(flip).wait_recv()
            for j in range(n_node):
                spot = (j // 2, j % 2)
                levz[(i,) + spot + (r,)] = (
                    levz[(i,) + spot + (r,)]
                    + level(zraw[(0,) + spot]) + level(zraw[(1,) + spot])
                )
            z_copy(p, 0).start()

        @pl.when(jnp.logical_not(end | near))
        def _():
            z_pass(0, 0)

    def z_ahead(k, h):
        @pl.when(end & (k < last))
        def _():
            p = piece(k)
            z_level(p, h, h == 0)
            z_copy(p, h).start()

    def z_finish():
        for h in range(2):
            z_level(z, h, h == 0)

            @pl.when(z > 0)
            def _():
                z_add(z, z, h)

            @pl.when(z < last)
            def _():
                z_add(z, n_z, h)

        for copy in z_first_copies():
            copy.start()

    def z_relay():
        for copy in z_first_copies():
            copy.wait_recv()
        for j in range(2):
            levz[intra, j, lo, z_part(0)] = levz[intra, j, lo, z_part(0)] + zfirst[0, j]
            levz[intra, hi, j, z_part(1)] = levz[intra, hi, j, z_part(1)] + zfirst[1, j]
        for copy in z_second_copies():
            copy.start()

    def give_third(k, s, lead=False):
        p = piece(k)
        second_sum(k, s, lead)
        via = k <= last - 2

        @pl.when(end & via)
        def _():
            agg_copy(k, s, lead).start()

        @pl.when(jnp.logical_not((end | near) & via))
        def _():
            third_copy(p, z, s, lead).start()

    def near_third(k, s, lead=False):
        @pl.when(near)
        def _():
            p = piece(k)
            i, r = p * CORES + core, rows_of(s, lead)
            agg_copy(k, s, lead).wait_recv()
            for h in range(2):
                lev[i, hi, lo, h, r] = lev[i, hi, lo, h, r] + agg[k, h, r]
            third_copy(p, z, s, lead).start()

    def begin():
        with scope("G0"):
            first_sum(1, 0)
            level_piece(2, 1)
            with scope("Gz"):
                z_inner(1, 0)
                z_inner(2, 0)
            z_ahead(2, 0)
            with scope("Gs"):
                give_third(0, 0, True)
            z_ahead(2, 1)
        with scope("G1"):
            first_sum(1, 1)
            level_piece(3, 0)
            with scope("Gz"):
                z_inner(1, 1)
                z_inner(2, 1)
            with scope("Gs"):
                give_third(0, 1, True)
            with scope("Gs"):
                give_third(1, 0)

    def middle(k, carry):
        with scope("M0"):
            first_sum(k, 0)
        with scope("M1"):
            first_sum(k, 1)
        level_piece(k + 1, 1)
        pl.when(k + 2 <= last)(lambda: level_piece(k + 2, 0))
        for h in range(2):
            z_ahead(k + 1, h)
            pl.when(k + 1 < last)(lambda: z_inner(k + 1, h))
        with scope("M3"):

            @pl.when(k == 2)
            def _():
                for s in range(SUBS):
                    near_third(0, s, True)

            @pl.when(k > 2)
            def _():
                for s in range(SUBS):
                    near_third(k - 2, s)

        with scope("M2"):
            give_third(k - 1, 1)
        with scope("Mz"):
            pl.when(k == last - 1)(z_finish)
        with scope("M4"):
            give_third(k, 0)
        return carry

    with scope("F0"):
        level_piece(0, 1, True)
        z_lead()
        level_piece(1, 0)
        for h in range(2):
            z_ahead(1, h)
        with scope("Fr"):
            raw_piece()
        level_piece(1, 1)
    with scope("F1"):
        with scope("Fz"):
            z_inner(0, 1)
        first_sum(0, 1, True)
        level_piece(2, 0)
    begin()
    factor = (ones * top_value) / (ones * (127.0 * float(n_dev) * scale_ref[0]))
    column = pl.multiple_of(node * BLOCK, BLOCK)
    own_signs = sign_tab[:, pl.ds(column, BLOCK)].astype(jnp.float32) * (factor * ROOT)
    for n in range(owned // SIGN_ROWS):
        sign_own[n * SIGN_ROWS : (n + 1) * SIGN_ROWS] = own_signs
    lax.fori_loop(2, last, middle, 0)
    with scope("H0"):
        first_sum(last, 0)
    with scope("H1"):
        give_third(last - 1, 1)
    with scope("H3"):
        first_sum(last, 1)
    with scope("H2"):
        for s in range(SUBS):
            near_third(last - 2, s)
    with scope("H4"):
        z_relay()
    with scope("K0"):
        second_sum(last, 0)
    with scope("K1"):
        second_sum(last, 1)

    def adam(start, summed):
        r = pl.ds(start, summed.shape[0])
        high = jnp.floor(summed * (1.0 / 64.0))
        low = summed - high * 64.0
        both = jnp.concatenate([high, low], axis=1).astype(jnp.bfloat16)
        grad = jnp.dot(both, split_bf[...], preferred_element_type=jnp.float32) * sign_own[r]
        new_first = 0.9 * first_in[r] + 0.1 * grad
        new_second = 0.95 * second_in[r] + 0.05 * grad * grad
        new_first_ref[r] = new_first
        new_second_ref[r] = new_second
        weights = weight_in[r]
        update = (new_first * first_unbias) / (jnp.sqrt(new_second * second_unbias) + 1e-08)
        new_weight_ref[r] = weights - 0.2 * (update + 0.1 * weights)

    def is_lead(other):
        return ((z == last) & (other < n_z // 2)) | ((z == 0) & (other >= n_z // 2))

    def direct(other):
        return jnp.logical_not(((other == 0) | (other == last)) & (jnp.abs(other - z) > 1))

    def from_plane(step, carry):
        other = lax.rem(z + step, n_z)
        for s in range(SUBS):
            for lead in (False, True):

                @pl.when(direct(other) & (is_lead(other) == lead))
                def _():
                    third_copy(other, other, s, lead).wait_recv()

        return carry

    def add_plane(step, carry):
        other = lax.rem(z + step, n_z)

        @pl.when(direct(other))
        def _():
            lev[intra, hi, lo] = lev[intra, hi, lo] + third[other]

        return carry

    with scope("L_third"):
        lax.fori_loop(1, n_z, from_plane, 0)
        lax.fori_loop(1, n_z, add_plane, 0)
    with scope("L_adam"):
        for h in range(2):
            adam(h * half, lev[intra, hi, lo, h])
    with scope("M_zlast"):
        for copy in z_second_copies():
            copy.wait_recv()
    with scope("M_adam"):
        adam(
            2 * half,
            jnp.concatenate(
                [levz[intra, hi, lo, z_part(h)] + zsecond[h] for h in range(2)], axis=0
            ),
        )

    def finish(k, carry):
        p = piece(k)
        pair_copy(p).wait_send()
        pairz_copy(p).wait_send()

        @pl.when(k > 0)
        def _():
            for s in range(SUBS):
                for copy in first_copies(p, s) + second_copies(p, s):
                    copy.wait_send()

        @pl.when(k < last)
        def _():
            z_copy(p, 1).wait_send()

        @pl.when((k < last) & jnp.logical_not(end & (k == 0)))
        def _():
            z_copy(p, 0).wait_send()

        def gave(lead):
            via = end & (k <= last - 2)
            for s in range(SUBS):
                pl.when(via)(lambda: agg_copy(k, s, lead).wait_send())
                pl.when(jnp.logical_not(via))(lambda: third_copy(p, z, s, lead).wait_send())

        pl.when(k == 0)(lambda: gave(True))
        pl.when((k > 0) & (k < last))(lambda: gave(False))

        return carry

    with scope("N_finish"):
        all_peaks().wait_send()
        for flip in range(2):
            for copy in raw_copies(flip):
                copy.wait_send()
        p = piece(0)
        for copy in first_copies(p, 1, True) + second_copies(p, 0, True) + second_copies(p, 1, True):
            copy.wait_send()

        @pl.when(end)
        def _():
            for flip in range(2):
                zraw_copy(flip).wait_send()

        lax.fori_loop(0, n_z, finish, 0)
        for copy in z_first_copies() + z_second_copies():
            copy.wait_send()


def store_kernel(*refs):
    sems = refs[-1]
    copies = [pltpu.make_async_copy(refs[n], refs[n + 3], sems.at[n]) for n in range(3)]
    for copy in copies:
        copy.start()
    for copy in copies:
        copy.wait()


def shards(gradients, sign_table, loss_scale, step_count, weights, first_moment, second_moment):
    n_node, n_intra = lax.axis_size("node"), lax.axis_size("intra")
    n_z = n_intra // CORES
    n_dev = n_node * n_intra
    local = gradients.reshape(gradients.shape[2:])
    rows, columns = local.shape
    owned = weights.shape[0]
    z_rows, half = plan_rows(owned)
    zh = z_rows // 2
    n_hi = n_node // 2
    anywhere = pl.BlockSpec(memory_space=pl.ANY)
    smem = pl.BlockSpec(memory_space=pltpu.SMEM)
    hbm = functools.partial(pltpu.with_memory_space_constraint, memory_space=pltpu.HBM)
    vmem = pl.BlockSpec(memory_space=pltpu.VMEM)
    dma = pltpu.SemaphoreType.DMA
    f32 = jnp.float32
    slots = min(SLOTS, n_intra)
    buffers = [
        ((slots, owned, columns), jnp.bfloat16),
        ((SIGN_ROWS, columns), jnp.int32),
        ((SIGN_ROWS, columns), jnp.bfloat16),
        ((WIDE, WIDE), jnp.bfloat16),
        ((WIDE, BLOCK), jnp.bfloat16),
    ] + [((owned, BLOCK), f32)] * 4
    large = [
        ((n_intra, n_hi, 2, 2, half, BLOCK), f32),
        ((n_intra, n_hi, 2, z_rows, BLOCK), f32),
        ((n_z, n_hi, 2, 2, half, BLOCK), f32),
        ((n_z, n_hi, 2, z_rows, BLOCK), f32),
        ((2, 2, 2, half * 8 // 10 // 8 * 8, BLOCK), f32),
        ((2, n_hi, 2, zh, BLOCK), f32),
        ((n_z, 2, 2, half, BLOCK), f32),
        ((n_z, 2, half, BLOCK), f32),
        ((n_z, 2, half, BLOCK), f32),
        ((n_z - 2, 2, half, BLOCK), f32),
        ((n_z + 1, n_hi, 2, z_rows, BLOCK), f32),
        ((2, 2, zh, BLOCK), f32),
        ((2, zh, BLOCK), f32),
        ((n_dev, 1, BLOCK), f32),
    ]
    held = sum(math.prod(shape) * jnp.dtype(kind).itemsize for shape, kind in buffers + large)
    shape = (owned, BLOCK)
    outs = pl.pallas_call(
        functools.partial(reduce_kernel, n_node, n_intra),
        out_shape=(pltpu.VMEM(shape, f32),) * 3,
        in_specs=[anywhere] * 2 + [smem] * 2 + [anywhere] * 3,
        out_specs=(vmem,) * 3,
        scratch_shapes=[pltpu.VMEM(*b) for b in buffers]
        + [pltpu.VMEM(*b) for b in large]
        + [
            dma((slots,)), dma((4,)),
            dma((n_z,)), dma((n_z,)), dma((n_z,)), dma((n_z,)),
            dma((2, 2)), dma((2, 2)), dma((2,)), dma((2,)),
            dma((2, n_z * SUBS)), dma((2, n_z * SUBS)),
            dma((2, n_z * SUBS)), dma((2, n_z * SUBS)),
            dma((n_z * SUBS,)), dma((n_z * SUBS,)),
            dma(((n_z - 2) * SUBS,)), dma(((n_z - 2) * SUBS,)),
            dma((n_z * 2,)), dma((n_z * 2 + 2,)),
            dma((2,)), dma((2,)), dma((2,)), dma((2,)),
            dma, dma,
        ],
        compiler_params=pltpu.CompilerParams(
            collective_id=0, has_side_effects=True, vmem_limit_bytes=held + (6 << 20)
        ),
    )(*(hbm(x) for x in (local, sign_table)), loss_scale, step_count,
      *(hbm(x) for x in (weights, first_moment, second_moment)))
    out = jax.ShapeDtypeStruct(shape, f32)
    return pl.pallas_call(
        store_kernel,
        out_shape=(out, out, out),
        in_specs=[vmem] * 3,
        out_specs=(anywhere,) * 3,
        scratch_shapes=[dma((3,))],
        compiler_params=pltpu.CompilerParams(vmem_limit_bytes=1 << 20),
    )(*outs)


def solution(mesh):
    own = P("intra", "node")
    return jax.shard_map(
        shards,
        mesh=mesh,
        in_specs=(P("node", "intra", None, None), P(), P(), P(), own, own, own),
        out_specs=(own, own, own),
        check_vma=False,
    )
```

```python
import contextlib
import functools
import math

import jax
import jax.numpy as jnp
from jax import lax
from jax.experimental import pallas as pl
from jax.experimental.pallas import tpu as pltpu
from jax.sharding import PartitionSpec as P

BLOCK = 128
WIDE = 2 * BLOCK
SIGN_ROWS = 64
CORES = 2
SLOTS = 8
SUBS = 2
ROOT = 1.0 / math.sqrt(BLOCK)
MESH = pl.DeviceIdType.MESH


def scope(name):
    return contextlib.nullcontext()


def parity_sign():
    shape = (BLOCK, BLOCK)
    parity = common = lax.broadcasted_iota(jnp.int32, shape, 0) & lax.broadcasted_iota(
        jnp.int32, shape, 1
    )
    for bit_index in range(1, BLOCK.bit_length() - 1):
        parity = parity ^ (common >> bit_index)
    return (1 - 2 * (parity & 1)).astype(jnp.float32)


def plan_rows(owned):
    z_rows = owned // 4 // 16 * 16
    return z_rows, (owned - z_rows) // 2


def reduce_kernel(
    n_node, n_intra, grad_ref, sign_ref, scale_ref, step_ref, weight_ref, first_ref, second_ref,
    new_weight_ref, new_first_ref, new_second_ref,
    stage, sign_tab, sign_bf, table_bf, split_bf, sign_own, weight_in, first_in, second_in, lev, levz, pair, pairz, raw, zraw, first, second, third, agg,
    zin, zfirst, zsecond, peaks,
    load_sem, side_sem, pair_send, pair_recv, pairz_send, pairz_recv, raw_send, raw_recv,
    zraw_send, zraw_recv, first_send, first_recv, second_send, second_recv, third_send, third_recv,
    agg_send, agg_recv, zin_send, zin_recv, zfirst_send, zfirst_recv, zsecond_send, zsecond_recv,
    peak_send, peak_recv,
):
    n_z = n_intra // CORES
    last = n_z - 1
    n_dev = n_node * n_intra
    owned = new_weight_ref.shape[0]
    z_rows, half = plan_rows(owned)
    zh = z_rows // 2
    cut = (half * 4 // 9) // 8 * 8
    spans = ((0, cut), (cut, half - cut))
    raw_rows = half * 8 // 10 // 8 * 8
    raw_spans = ((0, raw_rows), (raw_rows, half - raw_rows))
    node, intra = lax.axis_index("node"), lax.axis_index("intra")
    z, core = intra // CORES, intra % CORES
    hi, lo = node // 2, node % 2
    me = node * n_intra + intra
    end = (z == 0) | (z == last)
    near = (z == 1) | (z == last - 1)
    inward = jnp.where(z == 0, 1, last - 1)

    def at(node_index, z_index, core_index):
        return (node_index, z_index * CORES + core_index)

    def send(src, dst, send_sem, recv_sem, device):
        return pltpu.make_async_remote_copy(
            src_ref=src, dst_ref=dst, send_sem=send_sem, recv_sem=recv_sem,
            device_id=device, device_id_type=MESH,
        )

    def piece(k):
        lower = jnp.where(k < last - z, last - k, k - (last - z))
        upper = jnp.where(k < z, k, last - (k - z))
        return jnp.where(z < n_z // 2, lower, upper)

    def block_at(q):
        return piece(q // CORES) * CORES + jnp.where(q % CORES == 0, core, 1 - core)

    def load(q):
        slot = lax.rem(q, SLOTS)
        return pltpu.make_async_copy(
            grad_ref.at[pl.ds(block_at(q) * owned, owned)], stage.at[slot], load_sem.at[slot]
        )

    sides = [
        pltpu.make_async_copy(src, dst, side_sem.at[n])
        for n, (src, dst) in enumerate((
            (sign_ref, sign_tab), (weight_ref, weight_in), (first_ref, first_in), (second_ref, second_in),
        ))
    ]
    sides[0].start()
    for q in range(CORES):
        load(q).start()

    barrier = pltpu.get_barrier_semaphore()

    def everyone():
        for k in range(n_z):
            p = piece(k)
            for turn in range(n_node):
                other = lax.rem(node + turn, n_node)
                for flip in range(CORES):
                    if (k, turn, flip) != (last, 0, 0):
                        yield at(other, p, core if flip == 0 else 1 - core)

    for device in everyone():
        pl.semaphore_signal(barrier, inc=1, device_id=device, device_id_type=MESH)
    for q in range(CORES, min(SLOTS, n_intra)):
        load(q).start()
    table = parity_sign().astype(jnp.bfloat16)
    for a in range(2):
        for b in range(2):
            table_bf[a * BLOCK : (a + 1) * BLOCK, b * BLOCK : (b + 1) * BLOCK] = (
                table if a == b else jnp.zeros_like(table)
            )
    with scope("Asign"):
        sides[0].wait()
        sign_bf[...] = sign_tab[...].astype(jnp.float32).astype(jnp.bfloat16)

    def rotate(m, most):
        for q in range(CORES):
            load(m * CORES + q).wait()
        p = piece(m)
        blocks = [p * CORES + core, p * CORES + 1 - core]
        both_blocks = stage[pl.ds(lax.rem(m * CORES, SLOTS), CORES)].reshape(CORES * owned, -1)
        for w in range(n_node // 2):
            cols = slice(w * WIDE, (w + 1) * WIDE)
            part = both_blocks[:, cols].reshape(CORES * owned // SIGN_ROWS, SIGN_ROWS, WIDE)
            signed = (part * sign_bf[:, cols][None]).reshape(CORES * owned, WIDE)
            both = jnp.dot(signed, table_bf[...], preferred_element_type=jnp.float32)
            for c in range(CORES):
                for v in range(2):
                    spun = both[c * owned : (c + 1) * owned, v * BLOCK : (v + 1) * BLOCK]
                    for h in range(2):
                        lev[blocks[c], w, v, h] = spun[h * half : (h + 1) * half]
                    levz[blocks[c], w, v] = spun[2 * half :]
                    most = jnp.maximum(
                        most, jnp.max(jnp.abs(spun).reshape(owned // 8, 8, BLOCK), axis=0)
                    )
        for q in range(CORES):

            @pl.when(m * CORES + q + SLOTS < n_intra)
            def _():
                load(m * CORES + q + SLOTS).start()

        return most

    lo_peer = hi * 2 + 1 - lo
    hi_peer = (1 - hi) * 2 + lo

    def pair_copy(p):
        other = p * CORES + 1 - core
        return send(
            lev.at[other], pair.at[p], pair_send.at[p], pair_recv.at[p], at(node, z, 1 - core)
        )

    def pairz_copy(p):
        other = p * CORES + 1 - core
        return send(
            levz.at[other], pairz.at[p], pairz_send.at[p], pairz_recv.at[p], at(node, z, 1 - core)
        )

    def raw_copies(flip):
        target = core if flip == 0 else 1 - core
        i, r = piece(0) * CORES + target, pl.ds(0, raw_rows)
        return [
            send(
                src, raw.at[flip, h], raw_send.at[flip, h], raw_recv.at[flip, h],
                at(peer, z, target),
            )
            for h, src, peer in (
                (0, lev.at[i, :, 1 - lo, 0, r], lo_peer),
                (1, lev.at[i, 1 - hi, :, 1, r], hi_peer),
            )
        ]

    def zraw_copy(flip):
        target = core if flip == 0 else 1 - core
        return send(
            levz.at[piece(0) * CORES + target, :, :, z_part(0)], zraw.at[flip], zraw_send.at[flip], zraw_recv.at[flip],
            at(node, inward, target),
        )

    def rows_of(s, lead=False):
        return pl.ds(*(raw_spans if lead else spans)[s])

    def first_copies(p, s, lead=False):
        i, r = p * CORES + core, rows_of(s, lead)
        return [
            send(
                src, first.at[p, h, :, r], first_send.at[h, p * SUBS + s],
                first_recv.at[h, p * SUBS + s], at(peer, z, core),
            )
            for h, src, peer in (
                (0, lev.at[i, :, 1 - lo, 0, r], lo_peer),
                (1, lev.at[i, 1 - hi, :, 1, r], hi_peer),
            )
        ]

    def second_copies(p, s, lead=False):
        i, r = p * CORES + core, rows_of(s, lead)
        return [
            send(
                src, second.at[p, h, r], second_send.at[h, p * SUBS + s],
                second_recv.at[h, p * SUBS + s], at(peer, z, core),
            )
            for h, src, peer in (
                (0, lev.at[i, 1 - hi, lo, 0, r], hi_peer),
                (1, lev.at[i, hi, 1 - lo, 1, r], lo_peer),
            )
        ]

    def third_copy(p, slot, s, lead=False):
        r = rows_of(s, lead)
        return send(
            lev.at[p * CORES + core, hi, lo, :, r], third.at[slot, :, r],
            third_send.at[p * SUBS + s], third_recv.at[slot * SUBS + s], at(node, p, core),
        )

    def agg_copy(k, s, lead=False):
        r = rows_of(s, lead)
        return send(
            lev.at[piece(k) * CORES + core, hi, lo, :, r], agg.at[k, :, r],
            agg_send.at[k * SUBS + s], agg_recv.at[k * SUBS + s], at(node, inward, core),
        )

    def z_part(h):
        return pl.ds(h * zh, zh)

    def z_copy(p, h):
        onward = jnp.where(p > z, z + 1, z - 1)
        slot = jnp.where((p < z) & (p == onward), n_z, p)
        return send(
            levz.at[p * CORES + core, :, :, z_part(h)], zin.at[slot, :, :, z_part(h)],
            zin_send.at[p * 2 + h], zin_recv.at[slot * 2 + h], at(node, onward, core),
        )

    def z_arrived(slot, h):
        send(
            levz.at[core, :, :, z_part(h)], zin.at[slot, :, :, z_part(h)],
            zin_send.at[0], zin_recv.at[slot * 2 + h], at(node, inward, core),
        ).wait_recv()

    def z_first_copies():
        return [
            send(src, zfirst.at[h], zfirst_send.at[h], zfirst_recv.at[h], at(peer, z, core))
            for h, src, peer in (
                (0, levz.at[intra, :, 1 - lo, z_part(0)], lo_peer),
                (1, levz.at[intra, 1 - hi, :, z_part(1)], hi_peer),
            )
        ]

    def z_second_copies():
        return [
            send(src, zsecond.at[h], zsecond_send.at[h], zsecond_recv.at[h], at(peer, z, core))
            for h, src, peer in (
                (0, levz.at[intra, 1 - hi, lo, z_part(0)], hi_peer),
                (1, levz.at[intra, hi, 1 - lo, z_part(1)], lo_peer),
            )
        ]

    def peak_copy(device):
        return send(peaks.at[me], peaks.at[me], peak_send, peak_recv, device)

    def all_peaks():
        every = peaks.at[pl.ds(0, n_dev - 1)]
        return send(every, every, peak_send, peak_recv, at(node, z, 1 - core))

    with scope("A_rotate"):
        most = lax.fori_loop(0, n_z, rotate, jnp.zeros((8, BLOCK), jnp.float32))
        peaks[me] = jnp.max(most, axis=0, keepdims=True)
    for copy in sides[1:]:
        copy.start()
    with scope("B_barrier"):
        pl.semaphore_wait(barrier, n_dev - 1)

    with scope("C_issue"):
        for device in everyone():
            peak_copy(device).start()
        for flip in range(2):
            for copy in raw_copies(flip):
                copy.start()

        @pl.when(end)
        def _():
            for flip in range(2):
                zraw_copy(flip).start()

        def share(k, carry):
            pair_copy(piece(k)).start()
            pairz_copy(piece(k)).start()
            return carry

        lax.fori_loop(0, n_z, share, 0)

    with scope("D_sides"):
        for copy in sides[1:]:
            copy.wait()
        ones = jnp.ones((1, BLOCK), jnp.float32)
        steps = ones * step_ref[0].astype(jnp.float32)
        first_unbias = 1.0 / (1.0 - jnp.exp(steps * math.log(0.9)))
        second_unbias = 1.0 / (1.0 - jnp.exp(steps * math.log(0.95)))
        split_bf[0:BLOCK] = (parity_sign() * 64.0).astype(jnp.bfloat16)
        split_bf[BLOCK:] = parity_sign().astype(jnp.bfloat16)

    with scope("E_peaks"):
        all_peaks().wait_recv()
        tops = jnp.max(peaks[...], axis=0)
        top_value = jnp.max(tops, axis=1, keepdims=True) * ROOT
        level_scale = 127.0 / top_value

    def level(value):
        return jnp.floor((value * ROOT) * level_scale + 0.5)

    def level_piece(k, s, lead=False):
        p = piece(k)
        i, r = p * CORES + core, rows_of(s, lead)
        if lead or (s == 0):
            pair_copy(p).wait_recv()
        for j in range(n_node):
            for h in range(2):
                spot = (j // 2, j % 2, h, r)
                lev[(i,) + spot] = level(lev[(i,) + spot]) + level(pair[(p,) + spot])
        for copy in first_copies(p, s, lead):
            copy.start()

    def first_sum(k, s, lead=False):
        p = piece(k)
        i, r = p * CORES + core, rows_of(s, lead)
        for copy in first_copies(p, s, lead):
            copy.wait_recv()
        for j in range(2):
            lev[i, j, lo, 0, r] = lev[i, j, lo, 0, r] + first[p, 0, j, r]
            lev[i, hi, j, 1, r] = lev[i, hi, j, 1, r] + first[p, 1, j, r]
        for copy in second_copies(p, s, lead):
            copy.start()

    def second_sum(k, s, lead=False):
        p = piece(k)
        i, r = p * CORES + core, rows_of(s, lead)
        for copy in second_copies(p, s, lead):
            copy.wait_recv()
        for h in range(2):
            lev[i, hi, lo, h, r] = lev[i, hi, lo, h, r] + second[p, h, r]

    def raw_piece():
        p = piece(0)
        i, r = p * CORES + core, rows_of(0, True)
        for flip in range(2):
            for copy in raw_copies(flip):
                copy.wait_recv()

        def kept(h, j, spot):
            lev[(i,) + spot] = (
                level(lev[(i,) + spot]) + level(pair[(p,) + spot])
                + level(raw[0, h, j]) + level(raw[1, h, j])
            )

        for j in range(2):
            kept(0, j, (j, lo, 0, r))
            kept(1, j, (hi, j, 1, r))
        for copy in second_copies(p, 0, True):
            copy.start()

    def z_level(p, h, wait):
        i, r = p * CORES + core, z_part(h)
        if wait:
            pairz_copy(p).wait_recv()
        for j in range(n_node):
            spot = (j // 2, j % 2, r)
            levz[(i,) + spot] = level(levz[(i,) + spot]) + level(pairz[(p,) + spot])

    def z_add(p, slot, h):
        i, r = p * CORES + core, z_part(h)
        z_arrived(slot, h)
        for j in range(n_node):
            spot = (j // 2, j % 2, r)
            levz[(i,) + spot] = levz[(i,) + spot] + zin[(slot,) + spot]

    def z_pass(k, h):
        p = piece(k)
        z_level(p, h, h == 0)
        z_add(p, p, h)
        z_copy(p, h).start()

    def z_inner(k, h):
        @pl.when(jnp.logical_not(end))
        def _():
            z_pass(k, h)

    def z_lead():
        @pl.when(end)
        def _():
            z_level(piece(0), 1, True)
            z_copy(piece(0), 1).start()

        @pl.when(near)
        def _():
            p = piece(0)
            i, r = p * CORES + core, z_part(0)
            z_level(p, 0, True)
            for flip in range(2):
                zraw_copy(flip).wait_recv()
            for j in range(n_node):
                spot = (j // 2, j % 2)
                levz[(i,) + spot + (r,)] = (
                    levz[(i,) + spot + (r,)]
                    + level(zraw[(0,) + spot]) + level(zraw[(1,) + spot])
                )
            z_copy(p, 0).start()

        @pl.when(jnp.logical_not(end | near))
        def _():
            z_pass(0, 0)

    def z_ahead(k, h):
        @pl.when(end & (k < last))
        def _():
            p = piece(k)
            z_level(p, h, h == 0)
            z_copy(p, h).start()

    def z_finish():
        for h in range(2):
            z_level(z, h, h == 0)

            @pl.when(z > 0)
            def _():
                z_add(z, z, h)

            @pl.when(z < last)
            def _():
                z_add(z, n_z, h)

        for copy in z_first_copies():
            copy.start()

    def z_relay():
        for copy in z_first_copies():
            copy.wait_recv()
        for j in range(2):
            levz[intra, j, lo, z_part(0)] = levz[intra, j, lo, z_part(0)] + zfirst[0, j]
            levz[intra, hi, j, z_part(1)] = levz[intra, hi, j, z_part(1)] + zfirst[1, j]
        for copy in z_second_copies():
            copy.start()

    def give_third(k, s, lead=False):
        p = piece(k)
        second_sum(k, s, lead)
        via = k <= last - 2

        @pl.when(end & via)
        def _():
            agg_copy(k, s, lead).start()

        @pl.when(jnp.logical_not((end | near) & via))
        def _():
            third_copy(p, z, s, lead).start()

    def near_third(k, s, lead=False):
        @pl.when(near)
        def _():
            p = piece(k)
            i, r = p * CORES + core, rows_of(s, lead)
            agg_copy(k, s, lead).wait_recv()
            for h in range(2):
                lev[i, hi, lo, h, r] = lev[i, hi, lo, h, r] + agg[k, h, r]
            third_copy(p, z, s, lead).start()

    def begin():
        with scope("G0"):
            first_sum(1, 0)
            level_piece(2, 1)
            with scope("Gz"):
                z_inner(1, 0)
                z_inner(2, 0)
            z_ahead(2, 0)
            with scope("Gs"):
                give_third(0, 0, True)
            z_ahead(2, 1)
        with scope("G1"):
            first_sum(1, 1)
            level_piece(3, 0)
            with scope("Gz"):
                z_inner(1, 1)
                z_inner(2, 1)
            with scope("Gs"):
                give_third(0, 1, True)
            with scope("Gs"):
                give_third(1, 0)

    def middle(k, carry):
        with scope("M0"):
            first_sum(k, 0)
        with scope("M1"):
            first_sum(k, 1)
        level_piece(k + 1, 1)
        pl.when(k + 2 <= last)(lambda: level_piece(k + 2, 0))
        for h in range(2):
            z_ahead(k + 1, h)
            pl.when(k + 1 < last)(lambda: z_inner(k + 1, h))
        with scope("M3"):

            @pl.when(k == 2)
            def _():
                for s in range(SUBS):
                    near_third(0, s, True)

            @pl.when(k > 2)
            def _():
                for s in range(SUBS):
                    near_third(k - 2, s)

        with scope("M2"):
            give_third(k - 1, 1)
        with scope("M4"):
            give_third(k, 0)
        with scope("Mz"):
            pl.when(k == last - 1)(z_finish)
        return carry

    with scope("F0"):
        level_piece(0, 1, True)
        z_lead()
        level_piece(1, 0)
        for h in range(2):
            z_ahead(1, h)
        with scope("Fr"):
            raw_piece()
        level_piece(1, 1)
    with scope("F1"):
        with scope("Fz"):
            z_inner(0, 1)
        first_sum(0, 1, True)
        level_piece(2, 0)
    begin()
    factor = (ones * top_value) / (ones * (127.0 * float(n_dev) * scale_ref[0]))
    column = pl.multiple_of(node * BLOCK, BLOCK)
    own_signs = sign_tab[:, pl.ds(column, BLOCK)].astype(jnp.float32) * (factor * ROOT)
    for n in range(owned // SIGN_ROWS):
        sign_own[n * SIGN_ROWS : (n + 1) * SIGN_ROWS] = own_signs
    lax.fori_loop(2, last, middle, 0)
    with scope("H0"):
        first_sum(last, 0)
    with scope("H1"):
        give_third(last - 1, 1)
    with scope("H3"):
        first_sum(last, 1)
    with scope("H2"):
        for s in range(SUBS):
            near_third(last - 2, s)
    with scope("H4"):
        z_relay()
    with scope("K0"):
        second_sum(last, 0)
    with scope("K1"):
        second_sum(last, 1)

    def adam(start, summed):
        r = pl.ds(start, summed.shape[0])
        high = jnp.floor(summed * (1.0 / 64.0))
        low = summed - high * 64.0
        both = jnp.concatenate([high, low], axis=1).astype(jnp.bfloat16)
        grad = jnp.dot(both, split_bf[...], preferred_element_type=jnp.float32) * sign_own[r]
        new_first = 0.9 * first_in[r] + 0.1 * grad
        new_second = 0.95 * second_in[r] + 0.05 * grad * grad
        new_first_ref[r] = new_first
        new_second_ref[r] = new_second
        weights = weight_in[r]
        update = (new_first * first_unbias) / (jnp.sqrt(new_second * second_unbias) + 1e-08)
        new_weight_ref[r] = weights - 0.2 * (update + 0.1 * weights)

    def is_lead(other):
        return ((z == last) & (other < n_z // 2)) | ((z == 0) & (other >= n_z // 2))

    def direct(other):
        return jnp.logical_not(((other == 0) | (other == last)) & (jnp.abs(other - z) > 1))

    def from_plane(step, carry):
        other = lax.rem(z + step, n_z)
        for s in range(SUBS):
            for lead in (False, True):

                @pl.when(direct(other) & (is_lead(other) == lead))
                def _():
                    third_copy(other, other, s, lead).wait_recv()

        return carry

    def add_plane(step, carry):
        other = lax.rem(z + step, n_z)

        @pl.when(direct(other))
        def _():
            lev[intra, hi, lo] = lev[intra, hi, lo] + third[other]

        return carry

    with scope("L_third"):
        lax.fori_loop(1, n_z, from_plane, 0)
        lax.fori_loop(1, n_z, add_plane, 0)
    with scope("L_adam"):
        for h in range(2):
            adam(h * half, lev[intra, hi, lo, h])
    with scope("M_zlast"):
        for copy in z_second_copies():
            copy.wait_recv()
    with scope("M_adam"):
        adam(
            2 * half,
            jnp.concatenate(
                [levz[intra, hi, lo, z_part(h)] + zsecond[h] for h in range(2)], axis=0
            ),
        )

    def finish(k, carry):
        p = piece(k)
        pair_copy(p).wait_send()
        pairz_copy(p).wait_send()

        @pl.when(k > 0)
        def _():
            for s in range(SUBS):
                for copy in first_copies(p, s) + second_copies(p, s):
                    copy.wait_send()

        @pl.when(k < last)
        def _():
            z_copy(p, 1).wait_send()

        @pl.when((k < last) & jnp.logical_not(end & (k == 0)))
        def _():
            z_copy(p, 0).wait_send()

        def gave(lead):
            via = end & (k <= last - 2)
            for s in range(SUBS):
                pl.when(via)(lambda: agg_copy(k, s, lead).wait_send())
                pl.when(jnp.logical_not(via))(lambda: third_copy(p, z, s, lead).wait_send())

        pl.when(k == 0)(lambda: gave(True))
        pl.when((k > 0) & (k < last))(lambda: gave(False))

        return carry

    with scope("N_finish"):
        all_peaks().wait_send()
        for flip in range(2):
            for copy in raw_copies(flip):
                copy.wait_send()
        p = piece(0)
        for copy in first_copies(p, 1, True) + second_copies(p, 0, True) + second_copies(p, 1, True):
            copy.wait_send()

        @pl.when(end)
        def _():
            for flip in range(2):
                zraw_copy(flip).wait_send()

        lax.fori_loop(0, n_z, finish, 0)
        for copy in z_first_copies() + z_second_copies():
            copy.wait_send()


def store_kernel(*refs):
    sems = refs[-1]
    copies = [pltpu.make_async_copy(refs[n], refs[n + 3], sems.at[n]) for n in range(3)]
    for copy in copies:
        copy.start()
    for copy in copies:
        copy.wait()


def shards(gradients, sign_table, loss_scale, step_count, weights, first_moment, second_moment):
    n_node, n_intra = lax.axis_size("node"), lax.axis_size("intra")
    n_z = n_intra // CORES
    n_dev = n_node * n_intra
    local = gradients.reshape(gradients.shape[2:])
    rows, columns = local.shape
    owned = weights.shape[0]
    z_rows, half = plan_rows(owned)
    zh = z_rows // 2
    n_hi = n_node // 2
    anywhere = pl.BlockSpec(memory_space=pl.ANY)
    smem = pl.BlockSpec(memory_space=pltpu.SMEM)
    hbm = functools.partial(pltpu.with_memory_space_constraint, memory_space=pltpu.HBM)
    vmem = pl.BlockSpec(memory_space=pltpu.VMEM)
    dma = pltpu.SemaphoreType.DMA
    f32 = jnp.float32
    slots = min(SLOTS, n_intra)
    buffers = [
        ((slots, owned, columns), jnp.bfloat16),
        ((SIGN_ROWS, columns), jnp.int32),
        ((SIGN_ROWS, columns), jnp.bfloat16),
        ((WIDE, WIDE), jnp.bfloat16),
        ((WIDE, BLOCK), jnp.bfloat16),
    ] + [((owned, BLOCK), f32)] * 4
    large = [
        ((n_intra, n_hi, 2, 2, half, BLOCK), f32),
        ((n_intra, n_hi, 2, z_rows, BLOCK), f32),
        ((n_z, n_hi, 2, 2, half, BLOCK), f32),
        ((n_z, n_hi, 2, z_rows, BLOCK), f32),
        ((2, 2, 2, half * 8 // 10 // 8 * 8, BLOCK), f32),
        ((2, n_hi, 2, zh, BLOCK), f32),
        ((n_z, 2, 2, half, BLOCK), f32),
        ((n_z, 2, half, BLOCK), f32),
        ((n_z, 2, half, BLOCK), f32),
        ((n_z - 2, 2, half, BLOCK), f32),
        ((n_z + 1, n_hi, 2, z_rows, BLOCK), f32),
        ((2, 2, zh, BLOCK), f32),
        ((2, zh, BLOCK), f32),
        ((n_dev, 1, BLOCK), f32),
    ]
    held = sum(math.prod(shape) * jnp.dtype(kind).itemsize for shape, kind in buffers + large)
    shape = (owned, BLOCK)
    outs = pl.pallas_call(
        functools.partial(reduce_kernel, n_node, n_intra),
        out_shape=(pltpu.VMEM(shape, f32),) * 3,
        in_specs=[anywhere] * 2 + [smem] * 2 + [anywhere] * 3,
        out_specs=(vmem,) * 3,
        scratch_shapes=[pltpu.VMEM(*b) for b in buffers]
        + [pltpu.VMEM(*b) for b in large]
        + [
            dma((slots,)), dma((4,)),
            dma((n_z,)), dma((n_z,)), dma((n_z,)), dma((n_z,)),
            dma((2, 2)), dma((2, 2)), dma((2,)), dma((2,)),
            dma((2, n_z * SUBS)), dma((2, n_z * SUBS)),
            dma((2, n_z * SUBS)), dma((2, n_z * SUBS)),
            dma((n_z * SUBS,)), dma((n_z * SUBS,)),
            dma(((n_z - 2) * SUBS,)), dma(((n_z - 2) * SUBS,)),
            dma((n_z * 2,)), dma((n_z * 2 + 2,)),
            dma((2,)), dma((2,)), dma((2,)), dma((2,)),
            dma, dma,
        ],
        compiler_params=pltpu.CompilerParams(
            collective_id=0, has_side_effects=True, vmem_limit_bytes=held + (6 << 20)
        ),
    )(*(hbm(x) for x in (local, sign_table)), loss_scale, step_count,
      *(hbm(x) for x in (weights, first_moment, second_moment)))
    out = jax.ShapeDtypeStruct(shape, f32)
    return pl.pallas_call(
        store_kernel,
        out_shape=(out, out, out),
        in_specs=[vmem] * 3,
        out_specs=(anywhere,) * 3,
        scratch_shapes=[dma((3,))],
        compiler_params=pltpu.CompilerParams(vmem_limit_bytes=1 << 20),
    )(*outs)


def solution(mesh):
    own = P("intra", "node")
    return jax.shard_map(
        shards,
        mesh=mesh,
        in_specs=(P("node", "intra", None, None), P(), P(), P(), own, own, own),
        out_specs=(own, own, own),
        check_vma=False,
    )
```

```python
import contextlib
import functools
import math

import jax
import jax.numpy as jnp
from jax import lax
from jax.experimental import pallas as pl
from jax.experimental.pallas import tpu as pltpu
from jax.sharding import PartitionSpec as P

BLOCK = 128
WIDE = 2 * BLOCK
SIGN_ROWS = 64
CORES = 2
SLOTS = 8
SUBS = 2
ROOT = 1.0 / math.sqrt(BLOCK)
MESH = pl.DeviceIdType.MESH


def scope(name):
    return contextlib.nullcontext()


def parity_sign():
    shape = (BLOCK, BLOCK)
    parity = common = lax.broadcasted_iota(jnp.int32, shape, 0) & lax.broadcasted_iota(
        jnp.int32, shape, 1
    )
    for bit_index in range(1, BLOCK.bit_length() - 1):
        parity = parity ^ (common >> bit_index)
    return (1 - 2 * (parity & 1)).astype(jnp.float32)


def plan_rows(owned):
    z_rows = owned // 4 // 16 * 16
    return z_rows, (owned - z_rows) // 2


def reduce_kernel(
    n_node, n_intra, grad_ref, sign_ref, scale_ref, step_ref, weight_ref, first_ref, second_ref,
    new_weight_ref, new_first_ref, new_second_ref,
    stage, sign_tab, sign_bf, table_bf, split_bf, sign_own, weight_in, first_in, second_in, lev, levz, pair, pairz, raw, zraw, first, second, third, agg,
    zin, zfirst, zsecond, peaks,
    load_sem, side_sem, pair_send, pair_recv, pairz_send, pairz_recv, raw_send, raw_recv,
    zraw_send, zraw_recv, first_send, first_recv, second_send, second_recv, third_send, third_recv,
    agg_send, agg_recv, zin_send, zin_recv, zfirst_send, zfirst_recv, zsecond_send, zsecond_recv,
    peak_send, peak_recv,
):
    n_z = n_intra // CORES
    last = n_z - 1
    n_dev = n_node * n_intra
    owned = new_weight_ref.shape[0]
    z_rows, half = plan_rows(owned)
    zh = z_rows // 2
    cut = (half * 4 // 9) // 8 * 8
    spans = ((0, cut), (cut, half - cut))
    raw_rows = half * 8 // 10 // 8 * 8
    raw_spans = ((0, raw_rows), (raw_rows, half - raw_rows))
    node, intra = lax.axis_index("node"), lax.axis_index("intra")
    z, core = intra // CORES, intra % CORES
    hi, lo = node // 2, node % 2
    me = node * n_intra + intra
    end = (z == 0) | (z == last)
    near = (z == 1) | (z == last - 1)
    inward = jnp.where(z == 0, 1, last - 1)

    def at(node_index, z_index, core_index):
        return (node_index, z_index * CORES + core_index)

    def send(src, dst, send_sem, recv_sem, device):
        return pltpu.make_async_remote_copy(
            src_ref=src, dst_ref=dst, send_sem=send_sem, recv_sem=recv_sem,
            device_id=device, device_id_type=MESH,
        )

    def piece(k):
        lower = jnp.where(k < last - z, last - k, k - (last - z))
        upper = jnp.where(k < z, k, last - (k - z))
        return jnp.where(z < n_z // 2, lower, upper)

    def block_at(q):
        return piece(q // CORES) * CORES + jnp.where(q % CORES == 0, core, 1 - core)

    def load(q):
        slot = lax.rem(q, SLOTS)
        return pltpu.make_async_copy(
            grad_ref.at[pl.ds(block_at(q) * owned, owned)], stage.at[slot], load_sem.at[slot]
        )

    sides = [
        pltpu.make_async_copy(src, dst, side_sem.at[n])
        for n, (src, dst) in enumerate((
            (sign_ref, sign_tab), (weight_ref, weight_in), (first_ref, first_in), (second_ref, second_in),
        ))
    ]
    sides[0].start()
    for q in range(CORES):
        load(q).start()

    barrier = pltpu.get_barrier_semaphore()

    def everyone():
        for k in range(n_z):
            p = piece(k)
            for turn in range(n_node):
                other = lax.rem(node + turn, n_node)
                for flip in range(CORES):
                    if (k, turn, flip) != (last, 0, 0):
                        yield at(other, p, core if flip == 0 else 1 - core)

    for device in everyone():
        pl.semaphore_signal(barrier, inc=1, device_id=device, device_id_type=MESH)
    for q in range(CORES, min(SLOTS, n_intra)):
        load(q).start()
    table = parity_sign().astype(jnp.bfloat16)
    for a in range(2):
        for b in range(2):
            table_bf[a * BLOCK : (a + 1) * BLOCK, b * BLOCK : (b + 1) * BLOCK] = (
                table if a == b else jnp.zeros_like(table)
            )
    with scope("Asign"):
        sides[0].wait()
        sign_bf[...] = sign_tab[...].astype(jnp.float32).astype(jnp.bfloat16)

    def rotate(m, most):
        for q in range(CORES):
            load(m * CORES + q).wait()
        p = piece(m)
        blocks = [p * CORES + core, p * CORES + 1 - core]
        both_blocks = stage[pl.ds(lax.rem(m * CORES, SLOTS), CORES)].reshape(CORES * owned, -1)
        for w in range(n_node // 2):
            cols = slice(w * WIDE, (w + 1) * WIDE)
            part = both_blocks[:, cols].reshape(CORES * owned // SIGN_ROWS, SIGN_ROWS, WIDE)
            signed = (part * sign_bf[:, cols][None]).reshape(CORES * owned, WIDE)
            both = jnp.dot(signed, table_bf[...], preferred_element_type=jnp.float32)
            for c in range(CORES):
                for v in range(2):
                    spun = both[c * owned : (c + 1) * owned, v * BLOCK : (v + 1) * BLOCK]
                    for h in range(2):
                        lev[blocks[c], w, v, h] = spun[h * half : (h + 1) * half]
                    levz[blocks[c], w, v] = spun[2 * half :]
                    most = jnp.maximum(
                        most, jnp.max(jnp.abs(spun).reshape(owned // 8, 8, BLOCK), axis=0)
                    )
        for q in range(CORES):

            @pl.when(m * CORES + q + SLOTS < n_intra)
            def _():
                load(m * CORES + q + SLOTS).start()

        return most

    lo_peer = hi * 2 + 1 - lo
    hi_peer = (1 - hi) * 2 + lo

    def pair_copy(p):
        other = p * CORES + 1 - core
        return send(
            lev.at[other], pair.at[p], pair_send.at[p], pair_recv.at[p], at(node, z, 1 - core)
        )

    def pairz_copy(p):
        other = p * CORES + 1 - core
        return send(
            levz.at[other], pairz.at[p], pairz_send.at[p], pairz_recv.at[p], at(node, z, 1 - core)
        )

    def raw_copies(flip):
        target = core if flip == 0 else 1 - core
        i, r = piece(0) * CORES + target, pl.ds(0, raw_rows)
        return [
            send(
                src, raw.at[flip, h], raw_send.at[flip, h], raw_recv.at[flip, h],
                at(peer, z, target),
            )
            for h, src, peer in (
                (0, lev.at[i, :, 1 - lo, 0, r], lo_peer),
                (1, lev.at[i, 1 - hi, :, 1, r], hi_peer),
            )
        ]

    def zraw_copy(flip):
        target = core if flip == 0 else 1 - core
        return send(
            levz.at[piece(0) * CORES + target, :, :, z_part(0)], zraw.at[flip], zraw_send.at[flip], zraw_recv.at[flip],
            at(node, inward, target),
        )

    def rows_of(s, lead=False):
        return pl.ds(*(raw_spans if lead else spans)[s])

    def first_copies(p, s, lead=False):
        i, r = p * CORES + core, rows_of(s, lead)
        return [
            send(
                src, first.at[p, h, :, r], first_send.at[h, p * SUBS + s],
                first_recv.at[h, p * SUBS + s], at(peer, z, core),
            )
            for h, src, peer in (
                (0, lev.at[i, :, 1 - lo, 0, r], lo_peer),
                (1, lev.at[i, 1 - hi, :, 1, r], hi_peer),
            )
        ]

    def second_copies(p, s, lead=False):
        i, r = p * CORES + core, rows_of(s, lead)
        return [
            send(
                src, second.at[p, h, r], second_send.at[h, p * SUBS + s],
                second_recv.at[h, p * SUBS + s], at(peer, z, core),
            )
            for h, src, peer in (
                (0, lev.at[i, 1 - hi, lo, 0, r], hi_peer),
                (1, lev.at[i, hi, 1 - lo, 1, r], lo_peer),
            )
        ]

    def third_copy(p, slot, s, lead=False):
        r = rows_of(s, lead)
        return send(
            lev.at[p * CORES + core, hi, lo, :, r], third.at[slot, :, r],
            third_send.at[p * SUBS + s], third_recv.at[slot * SUBS + s], at(node, p, core),
        )

    def agg_copy(k, s, lead=False):
        r = rows_of(s, lead)
        return send(
            lev.at[piece(k) * CORES + core, hi, lo, :, r], agg.at[k, :, r],
            agg_send.at[k * SUBS + s], agg_recv.at[k * SUBS + s], at(node, inward, core),
        )

    def z_part(h):
        return pl.ds(h * zh, zh)

    def z_copy(p, h):
        onward = jnp.where(p > z, z + 1, z - 1)
        slot = jnp.where((p < z) & (p == onward), n_z, p)
        return send(
            levz.at[p * CORES + core, :, :, z_part(h)], zin.at[slot, :, :, z_part(h)],
            zin_send.at[p * 2 + h], zin_recv.at[slot * 2 + h], at(node, onward, core),
        )

    def z_arrived(slot, h):
        send(
            levz.at[core, :, :, z_part(h)], zin.at[slot, :, :, z_part(h)],
            zin_send.at[0], zin_recv.at[slot * 2 + h], at(node, inward, core),
        ).wait_recv()

    def z_first_copies():
        return [
            send(src, zfirst.at[h], zfirst_send.at[h], zfirst_recv.at[h], at(peer, z, core))
            for h, src, peer in (
                (0, levz.at[intra, :, 1 - lo, z_part(0)], lo_peer),
                (1, levz.at[intra, 1 - hi, :, z_part(1)], hi_peer),
            )
        ]

    def z_second_copies():
        return [
            send(src, zsecond.at[h], zsecond_send.at[h], zsecond_recv.at[h], at(peer, z, core))
            for h, src, peer in (
                (0, levz.at[intra, 1 - hi, lo, z_part(0)], hi_peer),
                (1, levz.at[intra, hi, 1 - lo, z_part(1)], lo_peer),
            )
        ]

    def peak_copy(device):
        return send(peaks.at[me], peaks.at[me], peak_send, peak_recv, device)

    def all_peaks():
        every = peaks.at[pl.ds(0, n_dev - 1)]
        return send(every, every, peak_send, peak_recv, at(node, z, 1 - core))

    with scope("A_rotate"):
        most = lax.fori_loop(0, n_z, rotate, jnp.zeros((8, BLOCK), jnp.float32))
        peaks[me] = jnp.max(most, axis=0, keepdims=True)
    for copy in sides[1:]:
        copy.start()
    with scope("B_barrier"):
        pl.semaphore_wait(barrier, n_dev - 1)

    with scope("C_issue"):
        for device in everyone():
            peak_copy(device).start()
        for flip in range(2):
            for copy in raw_copies(flip):
                copy.start()

        @pl.when(end)
        def _():
            for flip in range(2):
                zraw_copy(flip).start()

        def share(k, carry):
            pair_copy(piece(k)).start()
            pairz_copy(piece(k)).start()
            return carry

        lax.fori_loop(0, n_z, share, 0)

    with scope("D_sides"):
        for copy in sides[1:]:
            copy.wait()
        ones = jnp.ones((1, BLOCK), jnp.float32)
        steps = ones * step_ref[0].astype(jnp.float32)
        first_unbias = 1.0 / (1.0 - jnp.exp(steps * math.log(0.9)))
        second_unbias = 1.0 / (1.0 - jnp.exp(steps * math.log(0.95)))
        split_bf[0:BLOCK] = (parity_sign() * 64.0).astype(jnp.bfloat16)
        split_bf[BLOCK:] = parity_sign().astype(jnp.bfloat16)

    with scope("E_peaks"):
        all_peaks().wait_recv()
        tops = jnp.max(peaks[...], axis=0)
        top_value = jnp.max(tops, axis=1, keepdims=True) * ROOT
        level_scale = 127.0 / top_value

    def level(value):
        return jnp.floor((value * ROOT) * level_scale + 0.5)

    def level_piece(k, s, lead=False):
        p = piece(k)
        i, r = p * CORES + core, rows_of(s, lead)
        if lead or (s == 0):
            pair_copy(p).wait_recv()
        for j in range(n_node):
            for h in range(2):
                spot = (j // 2, j % 2, h, r)
                lev[(i,) + spot] = level(lev[(i,) + spot]) + level(pair[(p,) + spot])
        for copy in first_copies(p, s, lead):
            copy.start()

    def first_sum(k, s, lead=False):
        p = piece(k)
        i, r = p * CORES + core, rows_of(s, lead)
        for copy in first_copies(p, s, lead):
            copy.wait_recv()
        for j in range(2):
            lev[i, j, lo, 0, r] = lev[i, j, lo, 0, r] + first[p, 0, j, r]
            lev[i, hi, j, 1, r] = lev[i, hi, j, 1, r] + first[p, 1, j, r]
        for copy in second_copies(p, s, lead):
            copy.start()

    def second_sum(k, s, lead=False):
        p = piece(k)
        i, r = p * CORES + core, rows_of(s, lead)
        for copy in second_copies(p, s, lead):
            copy.wait_recv()
        for h in range(2):
            lev[i, hi, lo, h, r] = lev[i, hi, lo, h, r] + second[p, h, r]

    def raw_piece():
        p = piece(0)
        i, r = p * CORES + core, rows_of(0, True)
        for flip in range(2):
            for copy in raw_copies(flip):
                copy.wait_recv()

        def kept(h, j, spot):
            lev[(i,) + spot] = (
                level(lev[(i,) + spot]) + level(pair[(p,) + spot])
                + level(raw[0, h, j]) + level(raw[1, h, j])
            )

        for j in range(2):
            kept(0, j, (j, lo, 0, r))
            kept(1, j, (hi, j, 1, r))
        for copy in second_copies(p, 0, True):
            copy.start()

    def z_level(p, h, wait):
        i, r = p * CORES + core, z_part(h)
        if wait:
            pairz_copy(p).wait_recv()
        for j in range(n_node):
            spot = (j // 2, j % 2, r)
            levz[(i,) + spot] = level(levz[(i,) + spot]) + level(pairz[(p,) + spot])

    def z_add(p, slot, h):
        i, r = p * CORES + core, z_part(h)
        z_arrived(slot, h)
        for j in range(n_node):
            spot = (j // 2, j % 2, r)
            levz[(i,) + spot] = levz[(i,) + spot] + zin[(slot,) + spot]

    def z_pass(k, h):
        p = piece(k)
        z_level(p, h, h == 0)
        z_add(p, p, h)
        z_copy(p, h).start()

    def z_inner(k, h):
        @pl.when(jnp.logical_not(end))
        def _():
            z_pass(k, h)

    def z_lead():
        @pl.when(end)
        def _():
            z_level(piece(0), 1, True)
            z_copy(piece(0), 1).start()

        @pl.when(near)
        def _():
            p = piece(0)
            i, r = p * CORES + core, z_part(0)
            z_level(p, 0, True)
            for flip in range(2):
                zraw_copy(flip).wait_recv()
            for j in range(n_node):
                spot = (j // 2, j % 2)
                levz[(i,) + spot + (r,)] = (
                    levz[(i,) + spot + (r,)]
                    + level(zraw[(0,) + spot]) + level(zraw[(1,) + spot])
                )
            z_copy(p, 0).start()

        @pl.when(jnp.logical_not(end | near))
        def _():
            z_pass(0, 0)

    def z_ahead(k, h):
        @pl.when(end & (k < last))
        def _():
            p = piece(k)
            z_level(p, h, h == 0)
            z_copy(p, h).start()

    def z_finish():
        for h in range(2):
            z_level(z, h, h == 0)

            @pl.when(z > 0)
            def _():
                z_add(z, z, h)

            @pl.when(z < last)
            def _():
                z_add(z, n_z, h)

        for copy in z_first_copies():
            copy.start()

    def z_relay():
        for copy in z_first_copies():
            copy.wait_recv()
        for j in range(2):
            levz[intra, j, lo, z_part(0)] = levz[intra, j, lo, z_part(0)] + zfirst[0, j]
            levz[intra, hi, j, z_part(1)] = levz[intra, hi, j, z_part(1)] + zfirst[1, j]
        for copy in z_second_copies():
            copy.start()

    def give_third(k, s, lead=False):
        p = piece(k)
        second_sum(k, s, lead)
        via = k <= last - 2

        @pl.when(end & via)
        def _():
            agg_copy(k, s, lead).start()

        @pl.when(jnp.logical_not((end | near) & via))
        def _():
            third_copy(p, z, s, lead).start()

    def near_third(k, s, lead=False):
        @pl.when(near)
        def _():
            p = piece(k)
            i, r = p * CORES + core, rows_of(s, lead)
            agg_copy(k, s, lead).wait_recv()
            for h in range(2):
                lev[i, hi, lo, h, r] = lev[i, hi, lo, h, r] + agg[k, h, r]
            third_copy(p, z, s, lead).start()

    def begin():
        with scope("G0"):
            first_sum(1, 0)
            level_piece(2, 1)
            with scope("Gz"):
                z_inner(1, 0)
                z_inner(2, 0)
            z_ahead(2, 0)
            with scope("Gs"):
                give_third(0, 0, True)
            z_ahead(2, 1)
        with scope("G1"):
            first_sum(1, 1)
            level_piece(3, 0)
            with scope("Gz"):
                z_inner(1, 1)
                z_inner(2, 1)
            with scope("Gs"):
                give_third(0, 1, True)
            with scope("Gs"):
                give_third(1, 0)

    def middle(k, carry):
        with scope("M0"):
            first_sum(k, 0)
        with scope("M1"):
            first_sum(k, 1)
        level_piece(k + 1, 1)
        pl.when(k + 2 <= last)(lambda: level_piece(k + 2, 0))
        for h in range(2):
            z_ahead(k + 1, h)
            pl.when(k + 1 < last)(lambda: z_inner(k + 1, h))
        with scope("M3"):

            @pl.when(k == 2)
            def _():
                near_third(0, 0, True)

            @pl.when(k > 2)
            def _():
                for s in range(SUBS):
                    near_third(k - 2, s)

        with scope("M2"):
            give_third(k - 1, 1)
        @pl.when(k == 2)
        def _():
            near_third(0, 1, True)

        with scope("M4"):
            give_third(k, 0)
        with scope("Mz"):
            pl.when(k == last - 1)(z_finish)
        return carry

    with scope("F0"):
        level_piece(0, 1, True)
        z_lead()
        level_piece(1, 0)
        for h in range(2):
            z_ahead(1, h)
        with scope("Fr"):
            raw_piece()
        level_piece(1, 1)
    with scope("F1"):
        first_sum(0, 1, True)
        level_piece(2, 0)
        with scope("Fz"):
            z_inner(0, 1)
    begin()
    factor = (ones * top_value) / (ones * (127.0 * float(n_dev) * scale_ref[0]))
    column = pl.multiple_of(node * BLOCK, BLOCK)
    own_signs = sign_tab[:, pl.ds(column, BLOCK)].astype(jnp.float32) * (factor * ROOT)
    for n in range(owned // SIGN_ROWS):
        sign_own[n * SIGN_ROWS : (n + 1) * SIGN_ROWS] = own_signs
    lax.fori_loop(2, last, middle, 0)
    with scope("H0"):
        first_sum(last, 0)
    with scope("H1"):
        give_third(last - 1, 1)
    with scope("H3"):
        first_sum(last, 1)
    with scope("H2"):
        for s in range(SUBS):
            near_third(last - 2, s)
    with scope("H4"):
        z_relay()
    with scope("K0"):
        second_sum(last, 0)
    with scope("K1"):
        second_sum(last, 1)

    def adam(start, summed):
        r = pl.ds(start, summed.shape[0])
        high = jnp.floor(summed * (1.0 / 64.0))
        low = summed - high * 64.0
        both = jnp.concatenate([high, low], axis=1).astype(jnp.bfloat16)
        grad = jnp.dot(both, split_bf[...], preferred_element_type=jnp.float32) * sign_own[r]
        new_first = 0.9 * first_in[r] + 0.1 * grad
        new_second = 0.95 * second_in[r] + 0.05 * grad * grad
        new_first_ref[r] = new_first
        new_second_ref[r] = new_second
        weights = weight_in[r]
        update = (new_first * first_unbias) / (jnp.sqrt(new_second * second_unbias) + 1e-08)
        new_weight_ref[r] = weights - 0.2 * (update + 0.1 * weights)

    def is_lead(other):
        return ((z == last) & (other < n_z // 2)) | ((z == 0) & (other >= n_z // 2))

    def direct(other):
        return jnp.logical_not(((other == 0) | (other == last)) & (jnp.abs(other - z) > 1))

    def from_plane(step, carry):
        other = lax.rem(z + step, n_z)
        for s in range(SUBS):
            for lead in (False, True):

                @pl.when(direct(other) & (is_lead(other) == lead))
                def _():
                    third_copy(other, other, s, lead).wait_recv()

        return carry

    def add_plane(step, carry):
        other = lax.rem(z + step, n_z)

        @pl.when(direct(other))
        def _():
            lev[intra, hi, lo] = lev[intra, hi, lo] + third[other]

        return carry

    with scope("L_third"):
        lax.fori_loop(1, n_z, from_plane, 0)
        lax.fori_loop(1, n_z, add_plane, 0)
    with scope("L_adam"):
        for h in range(2):
            adam(h * half, lev[intra, hi, lo, h])
    with scope("M_zlast"):
        for copy in z_second_copies():
            copy.wait_recv()
    with scope("M_adam"):
        adam(
            2 * half,
            jnp.concatenate(
                [levz[intra, hi, lo, z_part(h)] + zsecond[h] for h in range(2)], axis=0
            ),
        )

    def finish(k, carry):
        p = piece(k)
        pair_copy(p).wait_send()
        pairz_copy(p).wait_send()

        @pl.when(k > 0)
        def _():
            for s in range(SUBS):
                for copy in first_copies(p, s) + second_copies(p, s):
                    copy.wait_send()

        @pl.when(k < last)
        def _():
            z_copy(p, 1).wait_send()

        @pl.when((k < last) & jnp.logical_not(end & (k == 0)))
        def _():
            z_copy(p, 0).wait_send()

        def gave(lead):
            via = end & (k <= last - 2)
            for s in range(SUBS):
                pl.when(via)(lambda: agg_copy(k, s, lead).wait_send())
                pl.when(jnp.logical_not(via))(lambda: third_copy(p, z, s, lead).wait_send())

        pl.when(k == 0)(lambda: gave(True))
        pl.when((k > 0) & (k < last))(lambda: gave(False))

        return carry

    with scope("N_finish"):
        all_peaks().wait_send()
        for flip in range(2):
            for copy in raw_copies(flip):
                copy.wait_send()
        p = piece(0)
        for copy in first_copies(p, 1, True) + second_copies(p, 0, True) + second_copies(p, 1, True):
            copy.wait_send()

        @pl.when(end)
        def _():
            for flip in range(2):
                zraw_copy(flip).wait_send()

        lax.fori_loop(0, n_z, finish, 0)
        for copy in z_first_copies() + z_second_copies():
            copy.wait_send()


def store_kernel(*refs):
    sems = refs[-1]
    copies = [pltpu.make_async_copy(refs[n], refs[n + 3], sems.at[n]) for n in range(3)]
    for copy in copies:
        copy.start()
    for copy in copies:
        copy.wait()


def shards(gradients, sign_table, loss_scale, step_count, weights, first_moment, second_moment):
    n_node, n_intra = lax.axis_size("node"), lax.axis_size("intra")
    n_z = n_intra // CORES
    n_dev = n_node * n_intra
    local = gradients.reshape(gradients.shape[2:])
    rows, columns = local.shape
    owned = weights.shape[0]
    z_rows, half = plan_rows(owned)
    zh = z_rows // 2
    n_hi = n_node // 2
    anywhere = pl.BlockSpec(memory_space=pl.ANY)
    smem = pl.BlockSpec(memory_space=pltpu.SMEM)
    hbm = functools.partial(pltpu.with_memory_space_constraint, memory_space=pltpu.HBM)
    vmem = pl.BlockSpec(memory_space=pltpu.VMEM)
    dma = pltpu.SemaphoreType.DMA
    f32 = jnp.float32
    slots = min(SLOTS, n_intra)
    buffers = [
        ((slots, owned, columns), jnp.bfloat16),
        ((SIGN_ROWS, columns), jnp.int32),
        ((SIGN_ROWS, columns), jnp.bfloat16),
        ((WIDE, WIDE), jnp.bfloat16),
        ((WIDE, BLOCK), jnp.bfloat16),
    ] + [((owned, BLOCK), f32)] * 4
    large = [
        ((n_intra, n_hi, 2, 2, half, BLOCK), f32),
        ((n_intra, n_hi, 2, z_rows, BLOCK), f32),
        ((n_z, n_hi, 2, 2, half, BLOCK), f32),
        ((n_z, n_hi, 2, z_rows, BLOCK), f32),
        ((2, 2, 2, half * 8 // 10 // 8 * 8, BLOCK), f32),
        ((2, n_hi, 2, zh, BLOCK), f32),
        ((n_z, 2, 2, half, BLOCK), f32),
        ((n_z, 2, half, BLOCK), f32),
        ((n_z, 2, half, BLOCK), f32),
        ((n_z - 2, 2, half, BLOCK), f32),
        ((n_z + 1, n_hi, 2, z_rows, BLOCK), f32),
        ((2, 2, zh, BLOCK), f32),
        ((2, zh, BLOCK), f32),
        ((n_dev, 1, BLOCK), f32),
    ]
    held = sum(math.prod(shape) * jnp.dtype(kind).itemsize for shape, kind in buffers + large)
    shape = (owned, BLOCK)
    outs = pl.pallas_call(
        functools.partial(reduce_kernel, n_node, n_intra),
        out_shape=(pltpu.VMEM(shape, f32),) * 3,
        in_specs=[anywhere] * 2 + [smem] * 2 + [anywhere] * 3,
        out_specs=(vmem,) * 3,
        scratch_shapes=[pltpu.VMEM(*b) for b in buffers]
        + [pltpu.VMEM(*b) for b in large]
        + [
            dma((slots,)), dma((4,)),
            dma((n_z,)), dma((n_z,)), dma((n_z,)), dma((n_z,)),
            dma((2, 2)), dma((2, 2)), dma((2,)), dma((2,)),
            dma((2, n_z * SUBS)), dma((2, n_z * SUBS)),
            dma((2, n_z * SUBS)), dma((2, n_z * SUBS)),
            dma((n_z * SUBS,)), dma((n_z * SUBS,)),
            dma(((n_z - 2) * SUBS,)), dma(((n_z - 2) * SUBS,)),
            dma((n_z * 2,)), dma((n_z * 2 + 2,)),
            dma((2,)), dma((2,)), dma((2,)), dma((2,)),
            dma, dma,
        ],
        compiler_params=pltpu.CompilerParams(
            collective_id=0, has_side_effects=True, vmem_limit_bytes=held + (6 << 20)
        ),
    )(*(hbm(x) for x in (local, sign_table)), loss_scale, step_count,
      *(hbm(x) for x in (weights, first_moment, second_moment)))
    out = jax.ShapeDtypeStruct(shape, f32)
    return pl.pallas_call(
        store_kernel,
        out_shape=(out, out, out),
        in_specs=[vmem] * 3,
        out_specs=(anywhere,) * 3,
        scratch_shapes=[dma((3,))],
        compiler_params=pltpu.CompilerParams(vmem_limit_bytes=1 << 20),
    )(*outs)


def solution(mesh):
    own = P("intra", "node")
    return jax.shard_map(
        shards,
        mesh=mesh,
        in_specs=(P("node", "intra", None, None), P(), P(), P(), own, own, own),
        out_specs=(own, own, own),
        check_vma=False,
    )
```

```python
import contextlib
import functools
import math

import jax
import jax.numpy as jnp
from jax import lax
from jax.experimental import pallas as pl
from jax.experimental.pallas import tpu as pltpu
from jax.sharding import PartitionSpec as P

BLOCK = 128
WIDE = 2 * BLOCK
SIGN_ROWS = 64
CORES = 2
SLOTS = 8
SUBS = 2
ROOT = 1.0 / math.sqrt(BLOCK)
MESH = pl.DeviceIdType.MESH


def scope(name):
    return contextlib.nullcontext()


def parity_sign():
    shape = (BLOCK, BLOCK)
    parity = common = lax.broadcasted_iota(jnp.int32, shape, 0) & lax.broadcasted_iota(
        jnp.int32, shape, 1
    )
    for bit_index in range(1, BLOCK.bit_length() - 1):
        parity = parity ^ (common >> bit_index)
    return (1 - 2 * (parity & 1)).astype(jnp.float32)


def plan_rows(owned):
    z_rows = owned // 4 // 16 * 16
    return z_rows, (owned - z_rows) // 2


def reduce_kernel(
    n_node, n_intra, grad_ref, sign_ref, scale_ref, step_ref, weight_ref, first_ref, second_ref,
    new_weight_ref, new_first_ref, new_second_ref,
    stage, sign_tab, sign_bf, table_bf, split_bf, sign_own, weight_in, first_in, second_in, lev, levz, pair, pairz, raw, zraw, first, second, third, agg,
    zin, zfirst, zsecond, peaks,
    load_sem, side_sem, pair_send, pair_recv, pairz_send, pairz_recv, raw_send, raw_recv,
    zraw_send, zraw_recv, first_send, first_recv, second_send, second_recv, third_send, third_recv,
    agg_send, agg_recv, zin_send, zin_recv, zfirst_send, zfirst_recv, zsecond_send, zsecond_recv,
    peak_send, peak_recv,
):
    n_z = n_intra // CORES
    last = n_z - 1
    n_dev = n_node * n_intra
    owned = new_weight_ref.shape[0]
    z_rows, half = plan_rows(owned)
    zh = z_rows // 2
    cut = (half * 4 // 9) // 8 * 8
    spans = ((0, cut), (cut, half - cut))
    raw_rows = half * 8 // 10 // 8 * 8
    raw_spans = ((0, raw_rows), (raw_rows, half - raw_rows))
    node, intra = lax.axis_index("node"), lax.axis_index("intra")
    z, core = intra // CORES, intra % CORES
    hi, lo = node // 2, node % 2
    me = node * n_intra + intra
    end = (z == 0) | (z == last)
    near = (z == 1) | (z == last - 1)
    inward = jnp.where(z == 0, 1, last - 1)

    def at(node_index, z_index, core_index):
        return (node_index, z_index * CORES + core_index)

    def send(src, dst, send_sem, recv_sem, device):
        return pltpu.make_async_remote_copy(
            src_ref=src, dst_ref=dst, send_sem=send_sem, recv_sem=recv_sem,
            device_id=device, device_id_type=MESH,
        )

    def piece(k):
        lower = jnp.where(k < last - z, last - k, k - (last - z))
        upper = jnp.where(k < z, k, last - (k - z))
        return jnp.where(z < n_z // 2, lower, upper)

    def block_at(q):
        return piece(q // CORES) * CORES + jnp.where(q % CORES == 0, core, 1 - core)

    def load(q):
        slot = lax.rem(q, SLOTS)
        return pltpu.make_async_copy(
            grad_ref.at[pl.ds(block_at(q) * owned, owned)], stage.at[slot], load_sem.at[slot]
        )

    sides = [
        pltpu.make_async_copy(src, dst, side_sem.at[n])
        for n, (src, dst) in enumerate((
            (sign_ref, sign_tab), (weight_ref, weight_in), (first_ref, first_in), (second_ref, second_in),
        ))
    ]
    sides[0].start()
    for q in range(CORES):
        load(q).start()

    barrier = pltpu.get_barrier_semaphore()

    def everyone():
        for k in range(n_z):
            p = piece(k)
            for turn in range(n_node):
                other = lax.rem(node + turn, n_node)
                for flip in range(CORES):
                    if (k, turn, flip) != (last, 0, 0):
                        yield at(other, p, core if flip == 0 else 1 - core)

    for device in everyone():
        pl.semaphore_signal(barrier, inc=1, device_id=device, device_id_type=MESH)
    for q in range(CORES, min(SLOTS, n_intra)):
        load(q).start()
    table = parity_sign().astype(jnp.bfloat16)
    for a in range(2):
        for b in range(2):
            table_bf[a * BLOCK : (a + 1) * BLOCK, b * BLOCK : (b + 1) * BLOCK] = (
                table if a == b else jnp.zeros_like(table)
            )
    with scope("Asign"):
        sides[0].wait()
        sign_bf[...] = sign_tab[...].astype(jnp.float32).astype(jnp.bfloat16)

    def rotate(m, most):
        for q in range(CORES):
            load(m * CORES + q).wait()
        p = piece(m)
        blocks = [p * CORES + core, p * CORES + 1 - core]
        both_blocks = stage[pl.ds(lax.rem(m * CORES, SLOTS), CORES)].reshape(CORES * owned, -1)
        for w in range(n_node // 2):
            cols = slice(w * WIDE, (w + 1) * WIDE)
            part = both_blocks[:, cols].reshape(CORES * owned // SIGN_ROWS, SIGN_ROWS, WIDE)
            signed = (part * sign_bf[:, cols][None]).reshape(CORES * owned, WIDE)
            both = jnp.dot(signed, table_bf[...], preferred_element_type=jnp.float32)
            for c in range(CORES):
                for v in range(2):
                    spun = both[c * owned : (c + 1) * owned, v * BLOCK : (v + 1) * BLOCK]
                    for h in range(2):
                        lev[blocks[c], w, v, h] = spun[h * half : (h + 1) * half]
                    levz[blocks[c], w, v] = spun[2 * half :]
                    most = jnp.maximum(
                        most, jnp.max(jnp.abs(spun).reshape(owned // 8, 8, BLOCK), axis=0)
                    )
        for q in range(CORES):

            @pl.when(m * CORES + q + SLOTS < n_intra)
            def _():
                load(m * CORES + q + SLOTS).start()

        return most

    lo_peer = hi * 2 + 1 - lo
    hi_peer = (1 - hi) * 2 + lo

    def pair_copy(p):
        other = p * CORES + 1 - core
        return send(
            lev.at[other], pair.at[p], pair_send.at[p], pair_recv.at[p], at(node, z, 1 - core)
        )

    def pairz_copy(p):
        other = p * CORES + 1 - core
        return send(
            levz.at[other], pairz.at[p], pairz_send.at[p], pairz_recv.at[p], at(node, z, 1 - core)
        )

    def raw_copies(flip):
        target = core if flip == 0 else 1 - core
        i, r = piece(0) * CORES + target, pl.ds(0, raw_rows)
        return [
            send(
                src, raw.at[flip, h], raw_send.at[flip, h], raw_recv.at[flip, h],
                at(peer, z, target),
            )
            for h, src, peer in (
                (0, lev.at[i, :, 1 - lo, 0, r], lo_peer),
                (1, lev.at[i, 1 - hi, :, 1, r], hi_peer),
            )
        ]

    def zraw_copy(flip):
        target = core if flip == 0 else 1 - core
        return send(
            levz.at[piece(0) * CORES + target, :, :, z_part(0)], zraw.at[flip], zraw_send.at[flip], zraw_recv.at[flip],
            at(node, inward, target),
        )

    def rows_of(s, lead=False):
        return pl.ds(*(raw_spans if lead else spans)[s])

    def first_copies(p, s, lead=False):
        i, r = p * CORES + core, rows_of(s, lead)
        return [
            send(
                src, first.at[p, h, :, r], first_send.at[h, p * SUBS + s],
                first_recv.at[h, p * SUBS + s], at(peer, z, core),
            )
            for h, src, peer in (
                (0, lev.at[i, :, 1 - lo, 0, r], lo_peer),
                (1, lev.at[i, 1 - hi, :, 1, r], hi_peer),
            )
        ]

    def second_copies(p, s, lead=False):
        i, r = p * CORES + core, rows_of(s, lead)
        return [
            send(
                src, second.at[p, h, r], second_send.at[h, p * SUBS + s],
                second_recv.at[h, p * SUBS + s], at(peer, z, core),
            )
            for h, src, peer in (
                (0, lev.at[i, 1 - hi, lo, 0, r], hi_peer),
                (1, lev.at[i, hi, 1 - lo, 1, r], lo_peer),
            )
        ]

    def third_copy(p, slot, s, lead=False):
        r = rows_of(s, lead)
        return send(
            lev.at[p * CORES + core, hi, lo, :, r], third.at[slot, :, r],
            third_send.at[p * SUBS + s], third_recv.at[slot * SUBS + s], at(node, p, core),
        )

    def agg_copy(k, s, lead=False):
        r = rows_of(s, lead)
        return send(
            lev.at[piece(k) * CORES + core, hi, lo, :, r], agg.at[k, :, r],
            agg_send.at[k * SUBS + s], agg_recv.at[k * SUBS + s], at(node, inward, core),
        )

    def z_part(h):
        return pl.ds(h * zh, zh)

    def z_copy(p, h):
        onward = jnp.where(p > z, z + 1, z - 1)
        slot = jnp.where((p < z) & (p == onward), n_z, p)
        return send(
            levz.at[p * CORES + core, :, :, z_part(h)], zin.at[slot, :, :, z_part(h)],
            zin_send.at[p * 2 + h], zin_recv.at[slot * 2 + h], at(node, onward, core),
        )

    def z_arrived(slot, h):
        send(
            levz.at[core, :, :, z_part(h)], zin.at[slot, :, :, z_part(h)],
            zin_send.at[0], zin_recv.at[slot * 2 + h], at(node, inward, core),
        ).wait_recv()

    def z_first_copies():
        return [
            send(src, zfirst.at[h], zfirst_send.at[h], zfirst_recv.at[h], at(peer, z, core))
            for h, src, peer in (
                (0, levz.at[intra, :, 1 - lo, z_part(0)], lo_peer),
                (1, levz.at[intra, 1 - hi, :, z_part(1)], hi_peer),
            )
        ]

    def z_second_copies():
        return [
            send(src, zsecond.at[h], zsecond_send.at[h], zsecond_recv.at[h], at(peer, z, core))
            for h, src, peer in (
                (0, levz.at[intra, 1 - hi, lo, z_part(0)], hi_peer),
                (1, levz.at[intra, hi, 1 - lo, z_part(1)], lo_peer),
            )
        ]

    def peak_copy(device):
        return send(peaks.at[me], peaks.at[me], peak_send, peak_recv, device)

    def all_peaks():
        every = peaks.at[pl.ds(0, n_dev - 1)]
        return send(every, every, peak_send, peak_recv, at(node, z, 1 - core))

    with scope("A_rotate"):
        most = lax.fori_loop(0, n_z, rotate, jnp.zeros((8, BLOCK), jnp.float32))
        peaks[me] = jnp.max(most, axis=0, keepdims=True)
    for copy in sides[1:]:
        copy.start()
    with scope("B_barrier"):
        pl.semaphore_wait(barrier, n_dev - 1)

    with scope("C_issue"):
        for device in everyone():
            peak_copy(device).start()
        for flip in range(2):
            for copy in raw_copies(flip):
                copy.start()

        @pl.when(end)
        def _():
            for flip in range(2):
                zraw_copy(flip).start()

        def share(k, carry):
            pair_copy(piece(k)).start()
            pairz_copy(piece(k)).start()
            return carry

        lax.fori_loop(0, n_z, share, 0)

    with scope("D_sides"):
        for copy in sides[1:]:
            copy.wait()
        ones = jnp.ones((1, BLOCK), jnp.float32)
        steps = ones * step_ref[0].astype(jnp.float32)
        first_unbias = 1.0 / (1.0 - jnp.exp(steps * math.log(0.9)))
        second_unbias = 1.0 / (1.0 - jnp.exp(steps * math.log(0.95)))
        split_bf[0:BLOCK] = (parity_sign() * 64.0).astype(jnp.bfloat16)
        split_bf[BLOCK:] = parity_sign().astype(jnp.bfloat16)

    with scope("E_peaks"):
        all_peaks().wait_recv()
        tops = jnp.max(peaks[...], axis=0)
        top_value = jnp.max(tops, axis=1, keepdims=True) * ROOT
        level_scale = 127.0 / top_value

    def level(value):
        return jnp.floor((value * ROOT) * level_scale + 0.5)

    def level_piece(k, s, lead=False):
        p = piece(k)
        i, r = p * CORES + core, rows_of(s, lead)
        if lead or (s == 0):
            pair_copy(p).wait_recv()
        for j in range(n_node):
            for h in range(2):
                spot = (j // 2, j % 2, h, r)
                lev[(i,) + spot] = level(lev[(i,) + spot]) + level(pair[(p,) + spot])
        for copy in first_copies(p, s, lead):
            copy.start()

    def first_sum(k, s, lead=False):
        p = piece(k)
        i, r = p * CORES + core, rows_of(s, lead)
        for copy in first_copies(p, s, lead):
            copy.wait_recv()
        for j in range(2):
            lev[i, j, lo, 0, r] = lev[i, j, lo, 0, r] + first[p, 0, j, r]
            lev[i, hi, j, 1, r] = lev[i, hi, j, 1, r] + first[p, 1, j, r]
        for copy in second_copies(p, s, lead):
            copy.start()

    def second_sum(k, s, lead=False):
        p = piece(k)
        i, r = p * CORES + core, rows_of(s, lead)
        for copy in second_copies(p, s, lead):
            copy.wait_recv()
        for h in range(2):
            lev[i, hi, lo, h, r] = lev[i, hi, lo, h, r] + second[p, h, r]

    def raw_piece():
        p = piece(0)
        i, r = p * CORES + core, rows_of(0, True)
        for flip in range(2):
            for copy in raw_copies(flip):
                copy.wait_recv()

        def kept(h, j, spot):
            lev[(i,) + spot] = (
                level(lev[(i,) + spot]) + level(pair[(p,) + spot])
                + level(raw[0, h, j]) + level(raw[1, h, j])
            )

        for j in range(2):
            kept(0, j, (j, lo, 0, r))
            kept(1, j, (hi, j, 1, r))
        for copy in second_copies(p, 0, True):
            copy.start()

    def z_level(p, h, wait):
        i, r = p * CORES + core, z_part(h)
        if wait:
            pairz_copy(p).wait_recv()
        for j in range(n_node):
            spot = (j // 2, j % 2, r)
            levz[(i,) + spot] = level(levz[(i,) + spot]) + level(pairz[(p,) + spot])

    def z_add(p, slot, h):
        i, r = p * CORES + core, z_part(h)
        z_arrived(slot, h)
        for j in range(n_node):
            spot = (j // 2, j % 2, r)
            levz[(i,) + spot] = levz[(i,) + spot] + zin[(slot,) + spot]

    def z_pass(k, h):
        p = piece(k)
        z_level(p, h, h == 0)
        z_add(p, p, h)
        z_copy(p, h).start()

    def z_inner(k, h):
        @pl.when(jnp.logical_not(end))
        def _():
            z_pass(k, h)

    def z_lead():
        @pl.when(end)
        def _():
            z_level(piece(0), 1, True)
            z_copy(piece(0), 1).start()

        @pl.when(near)
        def _():
            p = piece(0)
            i, r = p * CORES + core, z_part(0)
            z_level(p, 0, True)
            for flip in range(2):
                zraw_copy(flip).wait_recv()
            for j in range(n_node):
                spot = (j // 2, j % 2)
                levz[(i,) + spot + (r,)] = (
                    levz[(i,) + spot + (r,)]
                    + level(zraw[(0,) + spot]) + level(zraw[(1,) + spot])
                )
            z_copy(p, 0).start()

        @pl.when(jnp.logical_not(end | near))
        def _():
            z_pass(0, 0)

    def z_ahead(k, h):
        @pl.when(end & (k < last))
        def _():
            p = piece(k)
            z_level(p, h, h == 0)
            z_copy(p, h).start()

    def z_finish():
        for h in range(2):
            z_level(z, h, h == 0)

            @pl.when(z > 0)
            def _():
                z_add(z, z, h)

            @pl.when(z < last)
            def _():
                z_add(z, n_z, h)

        for copy in z_first_copies():
            copy.start()

    def z_relay():
        for copy in z_first_copies():
            copy.wait_recv()
        for j in range(2):
            levz[intra, j, lo, z_part(0)] = levz[intra, j, lo, z_part(0)] + zfirst[0, j]
            levz[intra, hi, j, z_part(1)] = levz[intra, hi, j, z_part(1)] + zfirst[1, j]
        for copy in z_second_copies():
            copy.start()

    def give_third(k, s, lead=False):
        p = piece(k)
        second_sum(k, s, lead)
        via = k <= last - 2

        @pl.when(end & via)
        def _():
            agg_copy(k, s, lead).start()

        @pl.when(jnp.logical_not((end | near) & via))
        def _():
            third_copy(p, z, s, lead).start()

    def near_third(k, s, lead=False):
        @pl.when(near)
        def _():
            p = piece(k)
            i, r = p * CORES + core, rows_of(s, lead)
            agg_copy(k, s, lead).wait_recv()
            for h in range(2):
                lev[i, hi, lo, h, r] = lev[i, hi, lo, h, r] + agg[k, h, r]
            third_copy(p, z, s, lead).start()

    def begin():
        with scope("G0"):
            first_sum(1, 0)
            level_piece(2, 1)
            with scope("Gz"):
                z_inner(1, 0)
                z_inner(2, 0)
            z_ahead(2, 0)
            with scope("Gs"):
                give_third(0, 0, True)
            z_ahead(2, 1)
        with scope("G1"):
            first_sum(1, 1)
            level_piece(3, 0)
            with scope("Gz"):
                z_inner(1, 1)
                z_inner(2, 1)
            with scope("Gs"):
                give_third(0, 1, True)
            with scope("Gs"):
                give_third(1, 0)

    def middle(k, carry):
        with scope("M0"):
            first_sum(k, 0)
        with scope("M1"):
            first_sum(k, 1)
        level_piece(k + 1, 1)
        pl.when(k + 2 <= last)(lambda: level_piece(k + 2, 0))
        for h in range(2):
            z_ahead(k + 1, h)
            pl.when(k + 1 < last)(lambda: z_inner(k + 1, h))
        with scope("M3"):

            @pl.when(k == 2)
            def _():
                for s in range(SUBS):
                    near_third(0, s, True)

            @pl.when(k > 2)
            def _():
                for s in range(SUBS):
                    near_third(k - 2, s)

        with scope("M2"):
            give_third(k - 1, 1)
        with scope("M4"):
            give_third(k, 0)
        with scope("Mz"):
            pl.when(k == last - 1)(z_finish)
        return carry

    with scope("F0"):
        level_piece(0, 1, True)
        z_lead()
        level_piece(1, 0)
        for h in range(2):
            z_ahead(1, h)
        with scope("Fr"):
            raw_piece()
        level_piece(1, 1)
    with scope("F1"):
        first_sum(0, 1, True)
        level_piece(2, 0)
        with scope("Fz"):
            z_inner(0, 1)
    begin()
    factor = (ones * top_value) / (ones * (127.0 * float(n_dev) * scale_ref[0]))
    column = pl.multiple_of(node * BLOCK, BLOCK)
    own_signs = sign_tab[:, pl.ds(column, BLOCK)].astype(jnp.float32) * (factor * ROOT)
    for n in range(owned // SIGN_ROWS):
        sign_own[n * SIGN_ROWS : (n + 1) * SIGN_ROWS] = own_signs
    lax.fori_loop(2, last, middle, 0)
    with scope("H0"):
        first_sum(last, 0)
    with scope("H1"):
        give_third(last - 1, 1)
    with scope("H3"):
        first_sum(last, 1)
    with scope("H2"):
        for s in range(SUBS):
            near_third(last - 2, s)
    with scope("H4"):
        z_relay()
    with scope("K0"):
        second_sum(last, 0)
    with scope("K1"):
        second_sum(last, 1)

    def adam(start, summed):
        r = pl.ds(start, summed.shape[0])
        high = jnp.floor(summed * (1.0 / 64.0))
        low = summed - high * 64.0
        both = jnp.concatenate([high, low], axis=1).astype(jnp.bfloat16)
        grad = jnp.dot(both, split_bf[...], preferred_element_type=jnp.float32) * sign_own[r]
        new_first = 0.9 * first_in[r] + 0.1 * grad
        new_second = 0.95 * second_in[r] + 0.05 * grad * grad
        new_first_ref[r] = new_first
        new_second_ref[r] = new_second
        weights = weight_in[r]
        update = (new_first * first_unbias) / (jnp.sqrt(new_second * second_unbias) + 1e-08)
        new_weight_ref[r] = weights - 0.2 * (update + 0.1 * weights)

    def is_lead(other):
        return ((z == last) & (other < n_z // 2)) | ((z == 0) & (other >= n_z // 2))

    def direct(other):
        return jnp.logical_not(((other == 0) | (other == last)) & (jnp.abs(other - z) > 1))

    def from_plane(step, carry):
        other = lax.rem(z + step, n_z)
        for s in range(SUBS):
            for lead in (False, True):

                @pl.when(direct(other) & (is_lead(other) == lead))
                def _():
                    third_copy(other, other, s, lead).wait_recv()

        return carry

    def add_plane(step, carry):
        other = lax.rem(z + step, n_z)

        @pl.when(direct(other))
        def _():
            lev[intra, hi, lo] = lev[intra, hi, lo] + third[other]

        return carry

    with scope("L_third"):
        lax.fori_loop(1, n_z, from_plane, 0)
        lax.fori_loop(1, n_z, add_plane, 0)
    with scope("L_adam"):
        for h in range(2):
            adam(h * half, lev[intra, hi, lo, h])
    with scope("M_zlast"):
        for copy in z_second_copies():
            copy.wait_recv()
    with scope("M_adam"):
        adam(
            2 * half,
            jnp.concatenate(
                [levz[intra, hi, lo, z_part(h)] + zsecond[h] for h in range(2)], axis=0
            ),
        )

    def finish(k, carry):
        p = piece(k)
        pair_copy(p).wait_send()
        pairz_copy(p).wait_send()

        @pl.when(k > 0)
        def _():
            for s in range(SUBS):
                for copy in first_copies(p, s) + second_copies(p, s):
                    copy.wait_send()

        @pl.when(k < last)
        def _():
            z_copy(p, 1).wait_send()

        @pl.when((k < last) & jnp.logical_not(end & (k == 0)))
        def _():
            z_copy(p, 0).wait_send()

        def gave(lead):
            via = end & (k <= last - 2)
            for s in range(SUBS):
                pl.when(via)(lambda: agg_copy(k, s, lead).wait_send())
                pl.when(jnp.logical_not(via))(lambda: third_copy(p, z, s, lead).wait_send())

        pl.when(k == 0)(lambda: gave(True))
        pl.when((k > 0) & (k < last))(lambda: gave(False))

        return carry

    with scope("N_finish"):
        all_peaks().wait_send()
        for flip in range(2):
            for copy in raw_copies(flip):
                copy.wait_send()
        p = piece(0)
        for copy in first_copies(p, 1, True) + second_copies(p, 0, True) + second_copies(p, 1, True):
            copy.wait_send()

        @pl.when(end)
        def _():
            for flip in range(2):
                zraw_copy(flip).wait_send()

        lax.fori_loop(0, n_z, finish, 0)
        for copy in z_first_copies() + z_second_copies():
            copy.wait_send()


def store_kernel(*refs):
    sems = refs[-1]
    half = refs[0].shape[0] // 2
    copies = [
        pltpu.make_async_copy(refs[n].at[r], refs[n + 3].at[r], sems.at[n, h])
        for h, r in enumerate((pl.ds(0, half), pl.ds(half, half)))
        for n in range(3)
    ]
    for copy in copies:
        copy.start()
    for copy in copies:
        copy.wait()


def shards(gradients, sign_table, loss_scale, step_count, weights, first_moment, second_moment):
    n_node, n_intra = lax.axis_size("node"), lax.axis_size("intra")
    n_z = n_intra // CORES
    n_dev = n_node * n_intra
    local = gradients.reshape(gradients.shape[2:])
    rows, columns = local.shape
    owned = weights.shape[0]
    z_rows, half = plan_rows(owned)
    zh = z_rows // 2
    n_hi = n_node // 2
    anywhere = pl.BlockSpec(memory_space=pl.ANY)
    smem = pl.BlockSpec(memory_space=pltpu.SMEM)
    hbm = functools.partial(pltpu.with_memory_space_constraint, memory_space=pltpu.HBM)
    vmem = pl.BlockSpec(memory_space=pltpu.VMEM)
    dma = pltpu.SemaphoreType.DMA
    f32 = jnp.float32
    slots = min(SLOTS, n_intra)
    buffers = [
        ((slots, owned, columns), jnp.bfloat16),
        ((SIGN_ROWS, columns), jnp.int32),
        ((SIGN_ROWS, columns), jnp.bfloat16),
        ((WIDE, WIDE), jnp.bfloat16),
        ((WIDE, BLOCK), jnp.bfloat16),
    ] + [((owned, BLOCK), f32)] * 4
    large = [
        ((n_intra, n_hi, 2, 2, half, BLOCK), f32),
        ((n_intra, n_hi, 2, z_rows, BLOCK), f32),
        ((n_z, n_hi, 2, 2, half, BLOCK), f32),
        ((n_z, n_hi, 2, z_rows, BLOCK), f32),
        ((2, 2, 2, half * 8 // 10 // 8 * 8, BLOCK), f32),
        ((2, n_hi, 2, zh, BLOCK), f32),
        ((n_z, 2, 2, half, BLOCK), f32),
        ((n_z, 2, half, BLOCK), f32),
        ((n_z, 2, half, BLOCK), f32),
        ((n_z - 2, 2, half, BLOCK), f32),
        ((n_z + 1, n_hi, 2, z_rows, BLOCK), f32),
        ((2, 2, zh, BLOCK), f32),
        ((2, zh, BLOCK), f32),
        ((n_dev, 1, BLOCK), f32),
    ]
    held = sum(math.prod(shape) * jnp.dtype(kind).itemsize for shape, kind in buffers + large)
    shape = (owned, BLOCK)
    outs = pl.pallas_call(
        functools.partial(reduce_kernel, n_node, n_intra),
        out_shape=(pltpu.VMEM(shape, f32),) * 3,
        in_specs=[anywhere] * 2 + [smem] * 2 + [anywhere] * 3,
        out_specs=(vmem,) * 3,
        scratch_shapes=[pltpu.VMEM(*b) for b in buffers]
        + [pltpu.VMEM(*b) for b in large]
        + [
            dma((slots,)), dma((4,)),
            dma((n_z,)), dma((n_z,)), dma((n_z,)), dma((n_z,)),
            dma((2, 2)), dma((2, 2)), dma((2,)), dma((2,)),
            dma((2, n_z * SUBS)), dma((2, n_z * SUBS)),
            dma((2, n_z * SUBS)), dma((2, n_z * SUBS)),
            dma((n_z * SUBS,)), dma((n_z * SUBS,)),
            dma(((n_z - 2) * SUBS,)), dma(((n_z - 2) * SUBS,)),
            dma((n_z * 2,)), dma((n_z * 2 + 2,)),
            dma((2,)), dma((2,)), dma((2,)), dma((2,)),
            dma, dma,
        ],
        compiler_params=pltpu.CompilerParams(
            collective_id=0, has_side_effects=True, vmem_limit_bytes=held + (6 << 20)
        ),
    )(*(hbm(x) for x in (local, sign_table)), loss_scale, step_count,
      *(hbm(x) for x in (weights, first_moment, second_moment)))
    out = jax.ShapeDtypeStruct(shape, f32)
    return pl.pallas_call(
        store_kernel,
        out_shape=(out, out, out),
        in_specs=[vmem] * 3,
        out_specs=(anywhere,) * 3,
        scratch_shapes=[dma((3, 2))],
        compiler_params=pltpu.CompilerParams(vmem_limit_bytes=1 << 20),
    )(*outs)


def solution(mesh):
    own = P("intra", "node")
    return jax.shard_map(
        shards,
        mesh=mesh,
        in_specs=(P("node", "intra", None, None), P(), P(), P(), own, own, own),
        out_specs=(own, own, own),
        check_vma=False,
    )
```
